32 devices in a mesh: gx: 8 (over y, x, core), gy: 4 (over z).
Axes of the slice: x: 2, y: 2, z: 4, core: 2. Of those that a mesh axis runs over, the one named last changes fastest.
Arguments:
- adjoint: float32 [9, 32, 128, 512], P(None, 'gx', 'gy'), may hold values from -6 to 6
- buoyancy: float32 [32, 128, 512], P('gx', 'gy'), may hold values from 0.5 to 2
- lame_lambda: float32 [32, 128, 512], P('gx', 'gy'), may hold values from 0.5 to 2
- shear_mu: float32 [32, 128, 512], P('gx', 'gy'), may hold values from 0.3 to 1.2
- packed: int32 [8, 8, 4, 12, 2048], P('gx', None, 'gy'), may hold values from -2147483648 to 2147483646
- scales: float32 [8, 8, 4, 12], P('gx', None, 'gy'), may hold values from 0.005 to 0.05
- perm: int32 [8, 8], P('gx'), may hold values from 0 to 7, each once within a row
Outputs:
- adjoint_out: float32 [9, 32, 128, 512], P(None, 'gx', 'gy')
- gradients: float32 [2, 32, 128, 512], P(None, 'gx', 'gy')
The draws below stay inside these ranges and needn't reach their ends.
Inputs may be any that keep to these rules, and one draw needn't show every extreme that they name: Each row of perm names every number 0 to 7 once. The words of packed are stored inputs and may cross devices as they are, four signed bytes to a word; only values that a program computes travel in float32.
All inputs are finite; a program needn't handle non-finite values.
Results may differ from the reference program's by a relative error of at most 0.0003.
Values sent between devices are 32-bit elements; how exact they have to be, the bound alone decides.
A program may use at most 128 MiB of HBM per device.

```python
import math
import jax
import jax.numpy as jnp
from jax import lax

CX = 4
CY = 32
CZ = 512
STEPS = 2
COMP = 12
OWNERS = 8
SEGW = 2048
NX = 32
NY = 128
NZ = 512
N_GY = 4


def place_ends(values, key, low, top_value):
    longest = values.shape.index(max(values.shape))
    spots = []
    for shift in (0, 1):
        where = [jax.random.randint(jax.random.fold_in(key, axis), (), 0, length) for axis, length in enumerate(values.shape)]
        where[longest] = (where[longest] + shift) % values.shape[longest]
        spots.append(tuple(where))
    return values.at[spots[0]].set(low).at[spots[1]].set(top_value)


def steps_of(stream_key, extent, cuts, low, top_value):
    loudness = 1.0
    for position, parts in cuts:
        draws = jax.random.uniform(jax.random.fold_in(jax.random.fold_in(stream_key, 6), position), (parts,), jnp.float32, low / len(cuts), top_value / len(cuts))
        loudness = loudness * jnp.repeat(jnp.exp(draws), extent[position] // parts).reshape((-1,) + (1,) * (len(extent) - 1 - position))
    return loudness


def normal_values(own_key, shape, spread, bound, cuts=(), kind=jnp.bfloat16):
    values = jax.random.normal(own_key, shape, jnp.float32) * spread
    if len(cuts) > 0:
        values = steps_of(own_key, shape, cuts, -0.22, 0.18) * values
    return jnp.clip(values, min=-bound, max=bound).astype(kind)


def setup_inputs(seed: int = 0) -> dict:
    keys = jax.random.split(jax.random.key(seed), 8)
    adjoint = normal_values(keys[0], (9, NX, NY, NZ), 1.0, 6.0, ((1, 8), (2, 4)), jnp.float32)
    buoyancy = jnp.clip(jnp.exp(math.log(2.0) - 1.3862944 * jax.random.uniform(keys[1], (NX, NY, NZ), jnp.float32) ** steps_of(keys[1], (NX, NY, NZ), ((0, 8), (1, 4)), -0.2, 0.2)), 0.5, 2.0)
    lame_lambda = jnp.clip(jnp.exp(math.log(2.0) - 1.3862944 * jax.random.uniform(keys[2], (NX, NY, NZ), jnp.float32) ** steps_of(keys[2], (NX, NY, NZ), ((0, 8), (1, 4)), -0.2, 0.2)), 0.5, 2.0)
    shear_mu = jnp.clip(jnp.exp(math.log(1.2) - 1.3862944 * jax.random.uniform(keys[3], (NX, NY, NZ), jnp.float32) ** steps_of(keys[3], (NX, NY, NZ), ((0, 8), (1, 4)), -0.2, 0.2)), 0.3, 1.2)
    packed = place_ends(jax.random.randint(keys[4], (OWNERS, OWNERS, N_GY, COMP, SEGW), -2147483648, 2147483647), jax.random.fold_in(keys[4], 1), -2147483648, 2147483646).astype(jnp.int32)
    scales = jnp.clip(jnp.exp(math.log(0.05) - 2.3025851 * jax.random.uniform(keys[5], (OWNERS, OWNERS, N_GY, COMP), jnp.float32) ** steps_of(keys[5], (OWNERS, OWNERS, N_GY, COMP), ((0, 8), (2, 4)), -0.2, 0.2)), 0.005, 0.05)
    perm = jax.vmap(lambda own: jax.random.permutation(own, OWNERS))(jax.random.split(keys[6], OWNERS)).reshape((OWNERS, OWNERS)).astype(jnp.int32)
    return dict(adjoint=adjoint, buoyancy=buoyancy, lame_lambda=lame_lambda, shear_mu=shear_mu, packed=packed, scales=scales, perm=perm)


courant = 0.15


def unpack(words):
    low = (words & 255) - 128
    middle = (jnp.right_shift(words, 8) & 255) - 128
    high = (jnp.right_shift(words, 16) & 255) - 128
    topmost = jnp.right_shift(words, 24)
    return jnp.concatenate([low, middle, high, topmost], axis=-1).astype(jnp.float32)


def inverse_order(row):
    count = row.shape[0]
    slots = jnp.arange(count, dtype=jnp.int32)
    hits = (row[None, :] == slots[:, None]).astype(jnp.int32)
    return jnp.sum(hits * slots[None, :], axis=1).astype(jnp.int32)


def forward_field(packed, scales, perm):
    comp = packed.shape[3]
    by_owner = jnp.swapaxes(packed, 0, 1)
    factors = jnp.swapaxes(scales, 0, 1)

    def one_owner(items):
        words, factor, row = items
        blocks = unpack(words) * factor[..., None]
        ordered = jnp.take(blocks, inverse_order(row), axis=0)
        return jnp.transpose(ordered, (2, 1, 0, 3)).reshape(comp, N_GY, CX, CY, CZ)

    whole_field = lax.map(one_owner, (by_owner, factors, perm))
    whole_field = jnp.transpose(whole_field, (1, 0, 3, 2, 4, 5))
    return whole_field.reshape(comp, NX, NY, NZ)


def step_ahead(field, axis):
    count = field.shape[axis]
    widths = [(0, 0)] * field.ndim
    widths[axis] = (0, 1)
    return jnp.pad(lax.slice_in_dim(field, 1, count, axis=axis), widths)


def step_behind(field, axis):
    count = field.shape[axis]
    widths = [(0, 0)] * field.ndim
    widths[axis] = (1, 0)
    return jnp.pad(lax.slice_in_dim(field, 0, count - 1, axis=axis), widths)


def diff_ahead(field, axis):
    return step_ahead(field, axis) - field


def diff_behind(field, axis):
    return field - step_behind(field, axis)


def move_velocity(velocity, stress, buoyancy):
    scaled = courant * buoyancy
    return [
        velocity[0] - scaled * (diff_ahead(stress[0], 0) + diff_behind(stress[3], 1) + diff_behind(stress[4], 2)),
        velocity[1] - scaled * (diff_behind(stress[3], 0) + diff_ahead(stress[1], 1) + diff_behind(stress[5], 2)),
        velocity[2] - scaled * (diff_behind(stress[4], 0) + diff_behind(stress[5], 1) + diff_ahead(stress[2], 2)),
    ]


def strains(velocity):
    return [
        diff_behind(velocity[0], 0),
        diff_behind(velocity[1], 1),
        diff_behind(velocity[2], 2),
        diff_ahead(velocity[0], 1) + diff_ahead(velocity[1], 0),
        diff_ahead(velocity[0], 2) + diff_ahead(velocity[2], 0),
        diff_ahead(velocity[1], 2) + diff_ahead(velocity[2], 1),
    ]


def move_stress(stress, strain, lame_lambda, shear_mu):
    trace = strain[0] + strain[1] + strain[2]
    result = []
    for index in range(3):
        result.append(stress[index] - courant * (lame_lambda * trace + 2.0 * shear_mu * strain[index]))
    for index in range(3, 6):
        result.append(stress[index] - courant * shear_mu * strain[index])
    return result


def reference(adjoint, buoyancy, lame_lambda, shear_mu, packed, scales, perm):
    forward = forward_field(packed, scales, perm)
    velocity = [adjoint[index] for index in range(3)]
    stress = [adjoint[index] for index in range(3, 9)]
    grad_lambda = jnp.zeros(buoyancy.shape, jnp.float32)
    grad_mu = jnp.zeros(buoyancy.shape, jnp.float32)
    for step in range(STEPS):
        velocity = move_velocity(velocity, stress, buoyancy)
        strain = strains(velocity)
        stress = move_stress(stress, strain, lame_lambda, shear_mu)
        stored = [forward[6 * step + index] for index in range(6)]
        trace = strain[0] + strain[1] + strain[2]
        grad_lambda = grad_lambda + trace * (stored[0] + stored[1] + stored[2])
        grad_mu = grad_mu + 2.0 * (strain[0] * stored[0] + strain[1] * stored[1] + strain[2] * stored[2])
        grad_mu = grad_mu + strain[3] * stored[3] + strain[4] * stored[4] + strain[5] * stored[5]
    return jnp.stack(velocity + stress), jnp.stack([grad_lambda, grad_mu])
```

```python
import functools

import jax
import jax.numpy as jnp
from jax import lax
from jax.experimental import pallas as pl
from jax.experimental.pallas import tpu as pltpu
from jax.sharding import PartitionSpec as P

MESH = pl.DeviceIdType.MESH
STEPS = 2
COURANT = 0.15
ROWS = 8
PIECES = 2
TURN = 6
GROUPS = (
    ((6, 0), (2, 0), (3, 0), (4, 0), (5, 0)),
    ((7, 0), (2, 1), (6, 1), (1, 0), (4, 1)),
    ((3, 1), (5, 1), (1, 1)),
    ((7, 1),),
)
RELAYS = ((), (0,), (), (1,))

VX, VY, VZ, SXX, SYY, SZZ, SXY, SXZ, SYZ = range(9)

STRESS_X = ((0, (SXX,), -1), (1, (SXY, SXZ), 1))
STRESS_Y = ((0, (SYY,), -1), (1, (SXY, SYZ), 1))
SPEED_X = ((3, (VY, VZ), -1), (5, (VX,), 1))
SPEED_Y = ((3, (VX, VZ), -1), (5, (VY,), 1))


def partner(me, distance, count):
    if count & (count - 1):
        return lax.rem(me + distance, count)
    result, bit = me, 1
    while bit < count:
        if distance & bit:
            result = result + bit - 2 * bit * ((me // bit) % 2)
        bit *= 2
    return result


def kernel(n_x, n_y, adj, buoy, lam, shear, packed, scales, perm_in, out, grads,
           cur, coef, strain, halo_y, send_y, relay, factors, factor_s, perm, inv,
           in_sem, rl_sem, rf_sem, xs_sem, xr_sem, ys_sem, yr_sem, ws_sem, wr_sem, fs_sem, fr_sem, loc_sem, *words):
    cx, cy, cz = buoy.shape
    comp = packed.shape[1]
    per_step = comp // STEPS
    lanes = packed.shape[3]
    segw = packed.shape[2] * lanes
    tiles = cy // ROWS
    pieces = xs_sem.shape[1]
    part = cy // pieces
    me_x, me_y = lax.axis_index("gx"), lax.axis_index("gy")

    loads = []

    def load(sem, source, target):
        copy = pltpu.make_async_copy(source, target, in_sem.at[sem])
        loads.append(copy)
        return copy

    edges = [load(12, adj.at[SXX, 0], cur.at[SXX, 1]),
             load(13, adj.at[pl.ds(SXY, 2), cx - 1], cur.at[pl.ds(SXY, 2), cx])]
    rows_in = [load(SYY, adj.at[SYY], cur.at[SYY, pl.ds(1, cx)]),
               load(SYZ, adj.at[SYZ], cur.at[SYZ, pl.ds(1, cx)]),
               load(SXY, adj.at[pl.ds(SXY, 2), pl.ds(0, cx - 1)], cur.at[pl.ds(SXY, 2), pl.ds(1, cx - 1)])]
    load(SXX, adj.at[SXX, pl.ds(1, cx - 1)], cur.at[SXX, pl.ds(2, cx - 1)])
    for index in (SZZ, VX, VY, VZ):
        load(index, adj.at[index], cur.at[index, pl.ds(1, cx)])
    for index, ref in enumerate((buoy, lam, shear)):
        load(9 + index, ref, coef.at[index])
    own_words = [pltpu.make_async_copy(packed.at[me_x, pl.ds(step * per_step, per_step)], words[step].at[me_x],
                                       loc_sem.at[2 + step]) for step in range(STEPS)]
    own_factor = pltpu.make_async_copy(scales.at[0, me_x], factors.at[me_x], loc_sem.at[1])
    for copy in loads[:len(edges)]:
        copy.start()

    barrier = pltpu.get_barrier_semaphore()
    for distance in range(1, n_x):
        pl.semaphore_signal(barrier, inc=1, device_id={"gx": partner(me_x, distance, n_x)}, device_id_type=MESH)

    def edge(way, axis):
        me, count = (me_x, n_x) if axis == "gx" else (me_y, n_y)
        return (me > 0) if way < 0 else (me < count - 1)

    for way in (-1, 1):
        @pl.when(edge(way, "gy"))
        def _():
            pl.semaphore_signal(barrier, inc=1, device_id={"gy": me_y + way}, device_id_type=MESH)

    for copy in loads[len(edges):]:
        copy.start()
    perm_copy = pltpu.make_async_copy(perm_in, perm, loc_sem.at[2 + STEPS])
    perm_copy.start()
    for copy in own_words:
        copy.start()
    own_factor.start()
    for way, place in ((-1, 0), (1, cx + 1)):
        @pl.when(jnp.logical_not(edge(way, "gx")))
        def _():
            for field in (VX, SXY, SXZ) if way < 0 else (VY, VZ, SXX):
                cur[field, place] = jnp.zeros((cy, cz), jnp.float32)

    pl.semaphore_wait(barrier, n_x - 1 + jnp.minimum(me_y, 1) + jnp.minimum(n_y - 1 - me_y, 1))

    def copy_x(step, message, piece):
        start, fields, way = message
        slot = 6 * step + start
        rows = pl.ds(piece * part, part)
        return pltpu.make_async_remote_copy(
            src_ref=cur.at[pl.ds(fields[0], len(fields)), 1 if way < 0 else cx, rows],
            dst_ref=cur.at[pl.ds(fields[0], len(fields)), cx + 1 if way < 0 else 0, rows],
            send_sem=xs_sem.at[slot, piece], recv_sem=xr_sem.at[slot, piece],
            device_id={"gx": me_x + way}, device_id_type=MESH)

    def copy_y(step, message):
        start, fields, way = message
        slot = 6 * step + start
        return pltpu.make_async_remote_copy(
            src_ref=send_y.at[pl.ds(slot, len(fields))], dst_ref=halo_y.at[pl.ds(slot, len(fields))],
            send_sem=ys_sem.at[slot], recv_sem=yr_sem.at[slot],
            device_id={"gy": me_y + way}, device_id_type=MESH)

    def word_copy(distance, step):
        to = partner(me_x, distance, n_x)
        stored = pl.ds(step * per_step, per_step)
        return pltpu.make_async_remote_copy(
            src_ref=packed.at[to, stored], dst_ref=words[step].at[me_x], send_sem=ws_sem.at[distance, step],
            recv_sem=wr_sem.at[distance, step], device_id={"gx": to}, device_id_type=MESH)

    def factor_copy(distance):
        to = partner(me_x, distance, n_x)
        return pltpu.make_async_remote_copy(
            src_ref=scales.at[0, to], dst_ref=factors.at[me_x], send_sem=fs_sem.at[distance],
            recv_sem=fr_sem.at[distance], device_id={"gx": to}, device_id_type=MESH)

    def send_x(step, messages, piece):
        for message in messages:
            @pl.when(edge(message[2], "gx"))
            def _():
                copy_x(step, message, piece).start()

    def send_rows(step, messages):
        for message in messages:
            start, fields, way = message

            @pl.when(edge(way, "gy"))
            def _():
                row = 0 if way < 0 else cy - 1
                for offset, field in enumerate(fields):
                    for x in range(cx):
                        send_y[6 * step + start + offset, pl.ds(x, 1), :] = cur[field, 1 + x, pl.ds(row, 1), :]
                copy_y(step, message).start()

    def finish_sends(step, messages_x, messages_y):
        for message in messages_x:
            @pl.when(edge(message[2], "gx"))
            def _():
                for piece in range(pieces):
                    copy_x(step, message, piece).wait_send()
        for message in messages_y:
            @pl.when(edge(message[2], "gy"))
            def _():
                copy_y(step, message).wait_send()

    def receive_y(step, messages):
        for message in messages:
            start, fields, way = message

            @pl.when(edge(-way, "gy"))
            def _():
                copy_y(step, message).wait_recv()

            @pl.when(jnp.logical_not(edge(-way, "gy")))
            def _():
                for offset in range(len(fields)):
                    halo_y[6 * step + start + offset] = jnp.zeros((cx, cz), jnp.float32)

    def receive_x(step, messages, piece):
        for message in messages:
            @pl.when(edge(-message[2], "gx"))
            def _():
                copy_x(step, message, piece).wait_recv()

    relays = n_x > TURN and n_x & (n_x - 1) == 0
    bent = (me_x // (TURN & -TURN)) % 2 != (me_x // (TURN - (TURN & -TURN))) % 2
    low, high = TURN & -TURN, TURN - (TURN & -TURN)

    def first_leg(step):
        return pltpu.make_async_remote_copy(
            src_ref=packed.at[partner(me_x, TURN, n_x), pl.ds(step * per_step, per_step)], dst_ref=relay.at[step],
            send_sem=ws_sem.at[TURN, step], recv_sem=rl_sem.at[step],
            device_id={"gx": partner(me_x, high, n_x)}, device_id_type=MESH)

    def second_leg(step):
        return pltpu.make_async_remote_copy(
            src_ref=relay.at[step], dst_ref=words[step].at[partner(me_x, high, n_x)],
            send_sem=rf_sem.at[step], recv_sem=wr_sem.at[TURN, step],
            device_id={"gx": partner(me_x, low, n_x)}, device_id_type=MESH)

    def send_group(which):
        for kind, step in GROUPS[which]:
            for distance in range(1, n_x):
                if max(distance * 8 // n_x, 1) == kind:
                    if relays and distance == TURN:
                        @pl.when(bent)
                        def _():
                            first_leg(step).start()

                        @pl.when(jnp.logical_not(bent))
                        def _():
                            word_copy(distance, step).start()
                    else:
                        word_copy(distance, step).start()
        if relays:
            for step in RELAYS[which]:
                @pl.when(jnp.logical_not(bent))
                def _():
                    first_leg(step).wait_recv()
                    second_leg(step).start()
        if which == 0:
            for distance in range(1, n_x):
                factor_copy(distance).start()

    def receive_words(step):
        if step == 0:
            own_factor.wait()
            for distance in range(1, n_x):
                factor_copy(distance).wait()
            to_scalar = pltpu.make_async_copy(factors, factor_s, loc_sem.at[0])
            to_scalar.start()
            to_scalar.wait()
        own_words[step].wait()
        for distance in range(1, n_x):
            word_copy(distance, step).wait()
        if relays:
            @pl.when(jnp.logical_not(bent))
            def _():
                second_leg(step).wait_send()

    sub = lax.broadcasted_iota(jnp.int32, (ROWS, cz), 0)
    lane = lax.broadcasted_iota(jnp.int32, (ROWS, cz), 1)
    first_row, last_row = sub == 0, sub == ROWS - 1
    first_lane, last_lane = lane == 0, lane == cz - 1

    def tile(field, x, t):
        return cur[field, x + 1, pl.ds(t * ROWS, ROWS), :]

    def z_before(value):
        return jnp.where(first_lane, 0.0, pltpu.roll(value, 1, 1))

    def z_after(value):
        return jnp.where(last_lane, 0.0, pltpu.roll(value, cz - 1, 1))

    def y_before(value, field, x, t, slot):
        row = halo_y[slot, pl.ds(x, 1), :] if t == 0 else cur[field, x + 1, pl.ds(t * ROWS - 1, 1), :]
        return jnp.where(first_row, jnp.broadcast_to(row, value.shape), pltpu.roll(value, 1, 0))

    def y_after(value, field, x, t, slot):
        row = halo_y[slot, pl.ds(x, 1), :] if t == tiles - 1 else cur[field, x + 1, pl.ds(t * ROWS + ROWS, 1), :]
        return jnp.where(last_row, jnp.broadcast_to(row, value.shape), pltpu.roll(value, ROWS - 1, 0))

    def velocity(step, which, x):
        slot = 6 * step
        for t in which:
            rows = pl.ds(t * ROWS, ROWS)
            scaled = COURANT * coef[0, x, rows, :]
            sxy, sxz, syz = tile(SXY, x, t), tile(SXZ, x, t), tile(SYZ, x, t)
            sxx, syy, szz = tile(SXX, x, t), tile(SYY, x, t), tile(SZZ, x, t)
            moved = (
                tile(VX, x, t) - scaled * (
                    (tile(SXX, x + 1, t) - sxx) + (sxy - y_before(sxy, SXY, x, t, slot + 1)) + (sxz - z_before(sxz))),
                tile(VY, x, t) - scaled * (
                    (sxy - tile(SXY, x - 1, t)) + (y_after(syy, SYY, x, t, slot) - syy) + (syz - z_before(syz))),
                tile(VZ, x, t) - scaled * (
                    (sxz - tile(SXZ, x - 1, t)) + (syz - y_before(syz, SYZ, x, t, slot + 2)) + (z_after(szz) - szz)))
            for field, value in enumerate(moved):
                cur[field, x + 1, rows, :] = value
                if step == STEPS - 1:
                    out[field, x, rows, :] = value

    def stress(step, which, x):
        slot = 6 * step + 3
        for t in which:
            rows = pl.ds(t * ROWS, ROWS)
            vx, vy, vz = tile(VX, x, t), tile(VY, x, t), tile(VZ, x, t)
            exx = vx - tile(VX, x - 1, t)
            eyy = vy - y_before(vy, VY, x, t, slot + 2)
            ezz = vz - z_before(vz)
            exy = (y_after(vx, VX, x, t, slot) - vx) + (tile(VY, x + 1, t) - vy)
            exz = (z_after(vx) - vx) + (tile(VZ, x + 1, t) - vz)
            eyz = (z_after(vy) - vy) + (y_after(vz, VZ, x, t, slot + 1) - vz)
            both = (exx, eyy, ezz, exy, exz, eyz)
            for index, value in enumerate(both):
                strain[6 * step + index, x, rows, :] = value
            pull = (COURANT * coef[1, x, rows, :]) * (exx + eyy + ezz)
            mu = COURANT * coef[2, x, rows, :]
            for index, value in enumerate(both):
                change = pull + (2.0 * mu) * value if index < 3 else mu * value
                moved = tile(SXX + index, x, t) - change
                if step == STEPS - 1:
                    out[SXX + index, x, rows, :] = moved
                else:
                    cur[SXX + index, x + 1, rows, :] = moved

    def over(first, last, body):
        def run(x, carry):
            body(x)
            return carry
        lax.fori_loop(first, last, run, 0)

    def ends(body):
        def run(index, carry):
            body(index * (cx - 1))
            return carry
        lax.fori_loop(0, 2, run, 0)

    width = lanes
    per_x = cy * cz // (4 * segw)

    def source(row, chunk):
        offset = row * cz + chunk * width
        within = offset % (4 * segw)
        return offset // (4 * segw), within % segw, within // segw

    sub_w = lax.broadcasted_iota(jnp.int32, (ROWS, width), 0)

    def gradient(step, x):
        made = {}
        for t in range(tiles):
            for chunk in range(cz // width):
                rows = pl.ds(t * ROWS, ROWS)
                columns = pl.ds(chunk * width, width)
                plan = [source(t * ROWS + r, chunk) for r in range(ROWS)]
                shift = jnp.full((ROWS, width), 8 * plan[0][2], jnp.int32)
                for r in range(1, ROWS):
                    if plan[r][2] != plan[r - 1][2]:
                        shift = jnp.where(sub_w >= r, 8 * plan[r][2], shift)
                key = tuple(p[:2] for p in plan)
                distinct = list(dict.fromkeys(key))
                masks = []
                for item in distinct[1:]:
                    mask = None
                    for r in range(ROWS):
                        if key[r] == item:
                            mask = (sub_w == r) if mask is None else mask | (sub_w == r)
                    masks.append(mask)
                holders = {b: inv[x * per_x + b] for b in dict.fromkeys(k[0] for k in key)}
                blocks = [k[0] for k in key]

                def stored(c):
                    if (key, c) not in made:
                        word = None
                        for position, (block, start) in enumerate(distinct):
                            piece = jnp.broadcast_to(
                                words[step][holders[block], c - per_step * step, pl.ds(start // lanes, 1), :], (ROWS, width))
                            word = piece if word is None else jnp.where(masks[position - 1], piece, word)
                        made[key, c] = word ^ jnp.int32(-2147483648)
                    byte = (lax.shift_right_logical(made[key, c], shift) & 255) - 128
                    factor = None
                    for r in range(ROWS):
                        if r == 0:
                            factor = factor_s[holders[blocks[0]], 0, c]
                        elif blocks[r] != blocks[r - 1]:
                            factor = jnp.where(sub_w >= r, factor_s[holders[blocks[r]], 0, c], factor)
                    return byte.astype(jnp.float32) * factor

                e = [strain[6 * step + index, x, rows, columns] for index in range(6)]
                f = [stored(6 * step + index) for index in range(6)]
                grad_lambda = (e[0] + e[1] + e[2]) * (f[0] + f[1] + f[2])
                grad_mu = 2.0 * (e[0] * f[0] + e[1] * f[1] + e[2] * f[2])
                grad_mu = grad_mu + e[3] * f[3] + e[4] * f[4] + e[5] * f[5]
                if step > 0:
                    grad_lambda = grads[0, x, rows, columns] + grad_lambda
                    grad_mu = grads[1, x, rows, columns] + grad_mu
                grads[0, x, rows, columns] = grad_lambda
                grads[1, x, rows, columns] = grad_mu

    def inside(piece):
        return range(piece * part // ROWS, (piece + 1) * part // ROWS)

    outer = (0, tiles - 1) if tiles > 1 else (0,)
    inner = range(1, tiles - 1)
    outside = [piece for piece in range(pieces) if set(inside(piece)) & set(outer)]
    within = [piece for piece in range(pieces) if piece not in outside]

    def phase(step, body, taken, taken_y, given_step, given, given_y):
        over(1, cx - 1, functools.partial(body, step, inner))
        for piece in within + outside:
            if piece == outside[0]:
                receive_y(step, taken_y)
            receive_x(step, taken, piece)
            ends(functools.partial(body, step, inside(piece)))
            if given:
                send_x(given_step, given, piece)
        over(1, cx - 1, functools.partial(body, step, outer))
        if given:
            send_rows(given_step, given_y)

    for copy in edges:
        copy.wait()
    for piece in within + outside:
        send_x(0, STRESS_X, piece)
    for copy in rows_in:
        copy.wait()
    send_rows(0, STRESS_Y)
    send_group(0)
    perm_copy.wait()

    def invert(block, carry):
        total = jnp.int32(0)
        for holder in range(n_x):
            total = jnp.where(perm[0, holder] == block, holder, total)
        inv[block] = total
        return carry
    lax.fori_loop(0, n_x, invert, 0)
    for copy in loads[len(edges) + len(rows_in):]:
        copy.wait()

    for step in range(STEPS):
        last = step == STEPS - 1
        if step > 0:
            finish_sends(step - 1, SPEED_X, SPEED_Y)
        phase(step, velocity, STRESS_X, STRESS_Y, step, SPEED_X, SPEED_Y)
        send_group(1 + 2 * step)
        if step > 0:
            receive_words(step - 1)
            over(0, cx, functools.partial(gradient, step - 1))
        finish_sends(step, STRESS_X, STRESS_Y)
        phase(step, stress, SPEED_X, SPEED_Y, step + 1, () if last else STRESS_X, STRESS_Y)
        if not last:
            send_group(2 + 2 * step)
    finish_sends(STEPS - 1, SPEED_X, SPEED_Y)
    receive_words(STEPS - 1)
    over(0, cx, functools.partial(gradient, STEPS - 1))


def flush(out_in, grads_in, out, grads, sem):
    copies = [pltpu.make_async_copy(out_in.at[index], out.at[index], sem.at[index]) for index in range(out.shape[0])]
    copies += [pltpu.make_async_copy(grads_in.at[index], grads.at[index], sem.at[out.shape[0] + index])
               for index in range(grads.shape[0])]
    for copy in copies:
        copy.start()
    for copy in copies:
        copy.wait()


def on_device(n_x, n_y, adjoint, buoyancy, lame_lambda, shear_mu, packed, scales, perm):
    fields, cx, cy, cz = adjoint.shape
    comp, segw = packed.shape[3:]
    lanes = min(128, segw)
    packed = packed.reshape(n_x, comp, segw // lanes, lanes)
    halos = 6 * STEPS
    pieces = PIECES if cy % (PIECES * ROWS) == 0 else 1
    dma = pltpu.SemaphoreType.DMA
    held = pl.pallas_call(
        functools.partial(kernel, n_x, n_y),
        out_shape=(pltpu.VMEM(adjoint.shape, jnp.float32), pltpu.VMEM((2, cx, cy, cz), jnp.float32)),
        in_specs=[pl.BlockSpec(memory_space=pltpu.HBM)] * 7,
        out_specs=(pl.BlockSpec(memory_space=pltpu.VMEM),) * 2,
        scratch_shapes=[
            pltpu.VMEM((fields, cx + 2, cy, cz), jnp.float32),
            pltpu.VMEM((3, cx, cy, cz), jnp.float32),
            pltpu.VMEM((comp, cx, cy, cz), jnp.float32),
            pltpu.VMEM((halos, cx, cz), jnp.float32),
            pltpu.VMEM((halos, cx, cz), jnp.float32),
            pltpu.VMEM((STEPS, comp // STEPS, segw // lanes, lanes), jnp.int32),
            pltpu.VMEM((n_x, 1, comp), jnp.float32),
            pltpu.SMEM((n_x, 1, comp), jnp.float32),
            pltpu.SMEM(perm.shape, jnp.int32),
            pltpu.SMEM((n_x,), jnp.int32),
            dma((14,)), dma((STEPS,)), dma((STEPS,)), dma((halos, pieces)), dma((halos, pieces)), dma((halos,)), dma((halos,)),
            dma((n_x, STEPS)), dma((n_x, STEPS)), dma((n_x,)), dma((n_x,)), dma((3 + STEPS,)),
        ] + [pltpu.VMEM((n_x, comp // STEPS, segw // lanes, lanes), jnp.int32)] * STEPS,
        compiler_params=pltpu.CompilerParams(collective_id=0, has_side_effects=True,
                                             vmem_limit_bytes=64000000),
    )(adjoint, buoyancy, lame_lambda, shear_mu, packed, scales, perm)
    return pl.pallas_call(
        flush,
        out_shape=tuple(jax.ShapeDtypeStruct(array.shape, jnp.float32) for array in held),
        in_specs=[pl.BlockSpec(memory_space=pltpu.VMEM)] * 2,
        out_specs=(pl.BlockSpec(memory_space=pltpu.HBM),) * 2,
        scratch_shapes=[dma((fields + 2,))],
        compiler_params=pltpu.CompilerParams(vmem_limit_bytes=1000000),
    )(*held)


def solution(mesh):
    return jax.shard_map(
        functools.partial(on_device, mesh.shape["gx"], mesh.shape["gy"]),
        mesh=mesh,
        in_specs=(
            P(None, "gx", "gy", None),
            P("gx", "gy", None),
            P("gx", "gy", None),
            P("gx", "gy", None),
            P("gx", None, "gy", None, None),
            P("gx", None, "gy", None),
            P("gx", None),
        ),
        out_specs=(P(None, "gx", "gy", None), P(None, "gx", "gy", None)),
        check_vma=False,
    )
```

```python
import functools

import jax
import jax.numpy as jnp
from jax import lax
from jax.experimental import pallas as pl
from jax.experimental.pallas import tpu as pltpu
from jax.sharding import PartitionSpec as P

MESH = pl.DeviceIdType.MESH
STEPS = 2
COURANT = 0.15
ROWS = 8
PIECES = 2
VMEM_LIMIT = 60500000
TURN = 6
BENT = (((6, 0), (4, 0), (5, 0), (2, 0), (3, 0)), ((6, 1), (7, 0), (2, 1), (1, 0)), ((4, 1), (5, 1), (3, 1), (7, 1), (1, 1)), ())
STRAIGHT = (((4, 0), (5, 0), (6, 0), (2, 0), (3, 0)), ((4, 1), (7, 0), (2, 1), (1, 0), (0, 0)), ((5, 1), (3, 1), (6, 1), (7, 1), (1, 1)), ((0, 1),))

VX, VY, VZ, SXX, SYY, SZZ, SXY, SXZ, SYZ = range(9)

STRESS_X = ((0, (SXX,), -1), (1, (SXY, SXZ), 1))
STRESS_Y = ((0, (SYY,), -1), (1, (SXY, SYZ), 1))
SPEED_X = ((3, (VY, VZ), -1), (5, (VX,), 1))
SPEED_Y = ((3, (VX, VZ), -1), (5, (VY,), 1))


def partner(me, distance, count):
    if count & (count - 1):
        return lax.rem(me + distance, count)
    result, bit = me, 1
    while bit < count:
        if distance & bit:
            result = result + bit - 2 * bit * ((me // bit) % 2)
        bit *= 2
    return result


def stencil(cur, coef, halo_y):
    cx, cy, cz = coef.shape[1:]
    tiles = cy // ROWS
    sub = lax.broadcasted_iota(jnp.int32, (ROWS, cz), 0)
    lane = lax.broadcasted_iota(jnp.int32, (ROWS, cz), 1)
    first_row, last_row = sub == 0, sub == ROWS - 1
    first_lane, last_lane = lane == 0, lane == cz - 1

    def tile(field, x, t):
        return cur[field, x + 1, pl.ds(t * ROWS, ROWS), :]

    def z_before(value):
        return jnp.where(first_lane, 0.0, pltpu.roll(value, 1, 1))

    def z_after(value):
        return jnp.where(last_lane, 0.0, pltpu.roll(value, cz - 1, 1))

    def y_before(value, field, x, t, slot):
        row = halo_y[slot, pl.ds(x, 1), :] if t == 0 else cur[field, x + 1, pl.ds(t * ROWS - 1, 1), :]
        return jnp.where(first_row, jnp.broadcast_to(row, value.shape), pltpu.roll(value, 1, 0))

    def y_after(value, field, x, t, slot):
        row = halo_y[slot, pl.ds(x, 1), :] if t == tiles - 1 else cur[field, x + 1, pl.ds(t * ROWS + ROWS, 1), :]
        return jnp.where(last_row, jnp.broadcast_to(row, value.shape), pltpu.roll(value, ROWS - 1, 0))

    def strains(step, x, t):
        slot = 6 * step + 3
        vx, vy, vz = tile(VX, x, t), tile(VY, x, t), tile(VZ, x, t)
        exx = vx - tile(VX, x - 1, t)
        eyy = vy - y_before(vy, VY, x, t, slot + 2)
        ezz = vz - z_before(vz)
        exy = (y_after(vx, VX, x, t, slot) - vx) + (tile(VY, x + 1, t) - vy)
        exz = (z_after(vx) - vx) + (tile(VZ, x + 1, t) - vz)
        eyz = (z_after(vy) - vy) + (y_after(vz, VZ, x, t, slot + 1) - vz)
        return exx, eyy, ezz, exy, exz, eyz

    def stresses(both, x, t):
        rows = pl.ds(t * ROWS, ROWS)
        exx, eyy, ezz = both[:3]
        pull = (COURANT * coef[1, x, rows, :]) * (exx + eyy + ezz)
        mu = COURANT * coef[2, x, rows, :]
        moved = []
        for index, value in enumerate(both):
            change = pull + (2.0 * mu) * value if index < 3 else mu * value
            moved.append(tile(SXX + index, x, t) - change)
        return moved

    return tile, z_before, z_after, y_before, y_after, strains, stresses


def products(e, f):
    grad_lambda = (e[0] + e[1] + e[2]) * (f[0] + f[1] + f[2])
    grad_mu = 2.0 * (e[0] * f[0] + e[1] * f[1] + e[2] * f[2])
    return grad_lambda, grad_mu + e[3] * f[3] + e[4] * f[4] + e[5] * f[5]


def kernel(n_x, n_y, adj, buoy, lam, shear, packed, scales, perm_in, cur, coef, halo_y, fwd, grads,
           strain, send_y, relay, factors, factor_s, perm, inv,
           in_sem, rl_sem, rf_sem, xs_sem, xr_sem, ys_sem, yr_sem, ws_sem, wr_sem, fs_sem, fr_sem, loc_sem, *words):
    cx, cy, cz = buoy.shape
    comp = packed.shape[1]
    per_step = comp // STEPS
    lanes = packed.shape[3]
    segw = packed.shape[2] * lanes
    tiles = cy // ROWS
    pieces = xs_sem.shape[1]
    part = cy // pieces
    me_x, me_y = lax.axis_index("gx"), lax.axis_index("gy")

    loads = []

    def load(sem, source, target):
        copy = pltpu.make_async_copy(source, target, in_sem.at[sem])
        loads.append(copy)
        return copy

    edges = [load(12, adj.at[SXX, 0], cur.at[SXX, 1]),
             load(13, adj.at[pl.ds(SXY, 2), cx - 1], cur.at[pl.ds(SXY, 2), cx])]
    rows_in = [load(SYY, adj.at[SYY], cur.at[SYY, pl.ds(1, cx)]),
               load(SYZ, adj.at[SYZ], cur.at[SYZ, pl.ds(1, cx)]),
               load(SXY, adj.at[pl.ds(SXY, 2), pl.ds(0, cx - 1)], cur.at[pl.ds(SXY, 2), pl.ds(1, cx - 1)])]
    load(SXX, adj.at[SXX, pl.ds(1, cx - 1)], cur.at[SXX, pl.ds(2, cx - 1)])
    for index in (SZZ, VX, VY, VZ):
        load(index, adj.at[index], cur.at[index, pl.ds(1, cx)])
    for index, ref in enumerate((buoy, lam, shear)):
        load(9 + index, ref, coef.at[index])
    own_words = [pltpu.make_async_copy(packed.at[me_x, pl.ds(step * per_step, per_step)], words[step].at[me_x],
                                       loc_sem.at[2 + step]) for step in range(STEPS)]
    own_factor = pltpu.make_async_copy(scales.at[0, me_x], factors.at[me_x], loc_sem.at[1])
    for copy in loads[:len(edges)]:
        copy.start()

    barrier = pltpu.get_barrier_semaphore()
    for distance in range(1, n_x):
        pl.semaphore_signal(barrier, inc=1, device_id={"gx": partner(me_x, distance, n_x)}, device_id_type=MESH)

    def edge(way, axis):
        me, count = (me_x, n_x) if axis == "gx" else (me_y, n_y)
        return (me > 0) if way < 0 else (me < count - 1)

    for way in (-1, 1):
        @pl.when(edge(way, "gy"))
        def _():
            pl.semaphore_signal(barrier, inc=1, device_id={"gy": me_y + way}, device_id_type=MESH)

    for copy in loads[len(edges):]:
        copy.start()
    perm_copy = pltpu.make_async_copy(perm_in, perm, loc_sem.at[2 + STEPS])
    perm_copy.start()
    for copy in own_words:
        copy.start()
    own_factor.start()
    for way, place in ((-1, 0), (1, cx + 1)):
        @pl.when(jnp.logical_not(edge(way, "gx")))
        def _():
            for field in (VX, SXY, SXZ) if way < 0 else (VY, VZ, SXX):
                cur[field, place] = jnp.zeros((cy, cz), jnp.float32)

    pl.semaphore_wait(barrier, n_x - 1 + jnp.minimum(me_y, 1) + jnp.minimum(n_y - 1 - me_y, 1))

    def copy_x(step, message, piece):
        start, fields, way = message
        slot = 6 * step + start
        rows = pl.ds(piece * part, part)
        return pltpu.make_async_remote_copy(
            src_ref=cur.at[pl.ds(fields[0], len(fields)), 1 if way < 0 else cx, rows],
            dst_ref=cur.at[pl.ds(fields[0], len(fields)), cx + 1 if way < 0 else 0, rows],
            send_sem=xs_sem.at[slot, piece], recv_sem=xr_sem.at[slot, piece],
            device_id={"gx": me_x + way}, device_id_type=MESH)

    def copy_y(step, message):
        start, fields, way = message
        slot = 6 * step + start
        return pltpu.make_async_remote_copy(
            src_ref=send_y.at[pl.ds(slot, len(fields))], dst_ref=halo_y.at[pl.ds(slot, len(fields))],
            send_sem=ys_sem.at[slot], recv_sem=yr_sem.at[slot],
            device_id={"gy": me_y + way}, device_id_type=MESH)

    def word_copy(distance, step):
        to = partner(me_x, distance, n_x)
        stored = pl.ds(step * per_step, per_step)
        return pltpu.make_async_remote_copy(
            src_ref=packed.at[to, stored], dst_ref=words[step].at[me_x], send_sem=ws_sem.at[distance, step],
            recv_sem=wr_sem.at[distance, step], device_id={"gx": to}, device_id_type=MESH)

    def factor_copy(distance):
        to = partner(me_x, distance, n_x)
        return pltpu.make_async_remote_copy(
            src_ref=scales.at[0, to], dst_ref=factors.at[me_x], send_sem=fs_sem.at[distance],
            recv_sem=fr_sem.at[distance], device_id={"gx": to}, device_id_type=MESH)

    def send_x(step, messages, piece):
        for message in messages:
            @pl.when(edge(message[2], "gx"))
            def _():
                copy_x(step, message, piece).start()

    def send_rows(step, messages):
        for message in messages:
            start, fields, way = message

            @pl.when(edge(way, "gy"))
            def _():
                row = 0 if way < 0 else cy - 1
                for offset, field in enumerate(fields):
                    for x in range(cx):
                        send_y[6 * step + start + offset, pl.ds(x, 1), :] = cur[field, 1 + x, pl.ds(row, 1), :]
                copy_y(step, message).start()

    def finish_sends(step, messages_x, messages_y):
        for message in messages_x:
            @pl.when(edge(message[2], "gx"))
            def _():
                for piece in range(pieces):
                    copy_x(step, message, piece).wait_send()
        for message in messages_y:
            @pl.when(edge(message[2], "gy"))
            def _():
                copy_y(step, message).wait_send()

    def receive_y(step, messages):
        for message in messages:
            start, fields, way = message

            @pl.when(edge(-way, "gy"))
            def _():
                copy_y(step, message).wait_recv()

            @pl.when(jnp.logical_not(edge(-way, "gy")))
            def _():
                for offset in range(len(fields)):
                    halo_y[6 * step + start + offset] = jnp.zeros((cx, cz), jnp.float32)

    def receive_x(step, messages, piece):
        for message in messages:
            @pl.when(edge(-message[2], "gx"))
            def _():
                copy_x(step, message, piece).wait_recv()

    relays = n_x > TURN and n_x & (n_x - 1) == 0
    bent = (me_x // (TURN & -TURN)) % 2 != (me_x // (TURN - (TURN & -TURN))) % 2
    low, high = TURN & -TURN, TURN - (TURN & -TURN)

    def first_leg(step):
        return pltpu.make_async_remote_copy(
            src_ref=packed.at[partner(me_x, TURN, n_x), pl.ds(step * per_step, per_step)], dst_ref=relay.at[step],
            send_sem=ws_sem.at[TURN, step], recv_sem=rl_sem.at[step],
            device_id={"gx": partner(me_x, high, n_x)}, device_id_type=MESH)

    def second_leg(step):
        return pltpu.make_async_remote_copy(
            src_ref=relay.at[step], dst_ref=words[step].at[partner(me_x, high, n_x)],
            send_sem=rf_sem.at[step], recv_sem=wr_sem.at[TURN, step],
            device_id={"gx": partner(me_x, low, n_x)}, device_id_type=MESH)

    def send_words(table, turned):
        for kind, step in table:
            if kind == 0 and relays:
                first_leg(step).wait_recv()
                second_leg(step).start()
            for distance in range(1, n_x):
                if max(distance * 8 // n_x, 1) == kind:
                    if turned and distance == TURN:
                        first_leg(step).start()
                    else:
                        word_copy(distance, step).start()

    def send_group(which):
        if relays:
            @pl.when(bent)
            def _():
                send_words(BENT[which], True)

            @pl.when(jnp.logical_not(bent))
            def _():
                send_words(STRAIGHT[which], False)
        else:
            send_words(STRAIGHT[which], False)
        if which == 0:
            for distance in range(1, n_x):
                factor_copy(distance).start()

    def receive_words(step):
        if step == 0:
            own_factor.wait()
            for distance in range(1, n_x):
                factor_copy(distance).wait()
            to_scalar = pltpu.make_async_copy(factors, factor_s, loc_sem.at[0])
            to_scalar.start()
            to_scalar.wait()
        own_words[step].wait()
        for distance in range(1, n_x):
            word_copy(distance, step).wait()
        if relays:
            @pl.when(jnp.logical_not(bent))
            def _():
                second_leg(step).wait_send()

    tile, z_before, z_after, y_before, y_after, strains, stresses = stencil(cur, coef, halo_y)

    def velocity(step, which, x):
        slot = 6 * step
        for t in which:
            rows = pl.ds(t * ROWS, ROWS)
            scaled = COURANT * coef[0, x, rows, :]
            sxy, sxz, syz = tile(SXY, x, t), tile(SXZ, x, t), tile(SYZ, x, t)
            sxx, syy, szz = tile(SXX, x, t), tile(SYY, x, t), tile(SZZ, x, t)
            moved = (
                tile(VX, x, t) - scaled * (
                    (tile(SXX, x + 1, t) - sxx) + (sxy - y_before(sxy, SXY, x, t, slot + 1)) + (sxz - z_before(sxz))),
                tile(VY, x, t) - scaled * (
                    (sxy - tile(SXY, x - 1, t)) + (y_after(syy, SYY, x, t, slot) - syy) + (syz - z_before(syz))),
                tile(VZ, x, t) - scaled * (
                    (sxz - tile(SXZ, x - 1, t)) + (syz - y_before(syz, SYZ, x, t, slot + 2)) + (z_after(szz) - szz)))
            for field, value in enumerate(moved):
                cur[field, x + 1, rows, :] = value

    def stress(step, which, x):
        for t in which:
            rows = pl.ds(t * ROWS, ROWS)
            both = strains(step, x, t)
            for index, value in enumerate(both):
                strain[6 * step + index, x, rows, :] = value
            for index, value in enumerate(stresses(both, x, t)):
                cur[SXX + index, x + 1, rows, :] = value

    def over(first, last, body):
        def run(x, carry):
            body(x)
            return carry
        lax.fori_loop(first, last, run, 0)

    def ends(body):
        def run(index, carry):
            body(index * (cx - 1))
            return carry
        lax.fori_loop(0, 2, run, 0)

    width = lanes
    per_x = cy * cz // (4 * segw)

    def source(row, chunk):
        offset = row * cz + chunk * width
        within = offset % (4 * segw)
        return offset // (4 * segw), within % segw, within // segw

    sub_w = lax.broadcasted_iota(jnp.int32, (ROWS, width), 0)

    def gradient(step, keep, x):
        made = {}
        for t in range(tiles):
            for chunk in range(cz // width):
                rows = pl.ds(t * ROWS, ROWS)
                columns = pl.ds(chunk * width, width)
                plan = [source(t * ROWS + r, chunk) for r in range(ROWS)]
                shift = jnp.full((ROWS, width), 8 * plan[0][2], jnp.int32)
                for r in range(1, ROWS):
                    if plan[r][2] != plan[r - 1][2]:
                        shift = jnp.where(sub_w >= r, 8 * plan[r][2], shift)
                key = tuple(p[:2] for p in plan)
                distinct = list(dict.fromkeys(key))
                masks = []
                for item in distinct[1:]:
                    mask = None
                    for r in range(ROWS):
                        if key[r] == item:
                            mask = (sub_w == r) if mask is None else mask | (sub_w == r)
                    masks.append(mask)
                holders = {b: inv[x * per_x + b] for b in dict.fromkeys(k[0] for k in key)}
                blocks = [k[0] for k in key]

                def stored(c):
                    if (key, c) not in made:
                        word = None
                        for position, (block, start) in enumerate(distinct):
                            piece = jnp.broadcast_to(
                                words[step][holders[block], c - per_step * step, pl.ds(start // lanes, 1), :], (ROWS, width))
                            word = piece if word is None else jnp.where(masks[position - 1], piece, word)
                        made[key, c] = word ^ jnp.int32(-2147483648)
                    byte = (lax.shift_right_logical(made[key, c], shift) & 255) - 128
                    factor = None
                    for r in range(ROWS):
                        if r == 0:
                            factor = factor_s[holders[blocks[0]], 0, c]
                        elif blocks[r] != blocks[r - 1]:
                            factor = jnp.where(sub_w >= r, factor_s[holders[blocks[r]], 0, c], factor)
                    return byte.astype(jnp.float32) * factor

                f = [stored(6 * step + index) for index in range(6)]
                if keep:
                    for index, value in enumerate(f):
                        fwd[index, x, rows, columns] = value
                else:
                    e = [strain[6 * step + index, x, rows, columns] for index in range(6)]
                    grad_lambda, grad_mu = products(e, f)
                    if step > 0:
                        grad_lambda = grads[0, x, rows, columns] + grad_lambda
                        grad_mu = grads[1, x, rows, columns] + grad_mu
                    grads[0, x, rows, columns] = grad_lambda
                    grads[1, x, rows, columns] = grad_mu

    def inside(piece):
        return range(piece * part // ROWS, (piece + 1) * part // ROWS)

    outer = (0, tiles - 1) if tiles > 1 else (0,)
    inner = range(1, tiles - 1)
    outside = [piece for piece in range(pieces) if set(inside(piece)) & set(outer)]
    within = [piece for piece in range(pieces) if piece not in outside]

    def phase(step, body, taken, taken_y, given_step, given, given_y, group):
        over(1, cx - 1, functools.partial(body, step, inner))
        receive_y(step, taken_y)
        over(1, cx - 1, functools.partial(body, step, outer))
        for piece in within + outside:
            receive_x(step, taken, piece)
            ends(functools.partial(body, step, inside(piece)))
            send_x(given_step, given, piece)
        send_rows(given_step, given_y)
        send_group(group)

    for copy in edges:
        copy.wait()
    for piece in within + outside:
        send_x(0, STRESS_X, piece)
    send_group(0)
    for copy in rows_in:
        copy.wait()
    send_rows(0, STRESS_Y)
    perm_copy.wait()

    def invert(block, carry):
        total = jnp.int32(0)
        for holder in range(n_x):
            total = jnp.where(perm[0, holder] == block, holder, total)
        inv[block] = total
        return carry
    lax.fori_loop(0, n_x, invert, 0)
    for copy in loads[len(edges) + len(rows_in):]:
        copy.wait()

    final = STEPS - 1
    for step in range(STEPS):
        if step > 0:
            finish_sends(step - 1, SPEED_X, SPEED_Y)
        phase(step, velocity, STRESS_X, STRESS_Y, step, SPEED_X, SPEED_Y, 1 + 2 * step)
        if step > 0:
            receive_words(step - 1)
            over(0, cx, functools.partial(gradient, step - 1, False))
        finish_sends(step, STRESS_X, STRESS_Y)
        if step < final:
            phase(step, stress, SPEED_X, SPEED_Y, step + 1, STRESS_X, STRESS_Y, 2 + 2 * step)
    over(1, cx - 1, functools.partial(stress, final, inner))
    receive_y(final, SPEED_Y)
    over(1, cx - 1, functools.partial(stress, final, outer))
    receive_words(final)
    over(1, cx - 1, functools.partial(gradient, final, False))
    ends(functools.partial(gradient, final, True))
    for piece in within + outside:
        receive_x(final, SPEED_X, piece)
    finish_sends(final, SPEED_X, SPEED_Y)


def finish(cur, coef, halo_y, fwd, grads_in, out, grads, s_end, g_end, sem):
    cx, cy, cz = coef.shape[1:]
    tile, z_before, z_after, y_before, y_after, strains, stresses = stencil(cur, coef, halo_y)
    copies = []

    def send(source, target):
        copies.append(pltpu.make_async_copy(source, target, sem.at[len(copies)]))
        copies[-1].start()

    for field in (VX, VY, VZ):
        send(cur.at[field, pl.ds(1, cx)], out.at[field])
    middle = pl.ds(1, cx - 2)
    send(cur.at[pl.ds(SXX, 6), pl.ds(2, cx - 2)], out.at[pl.ds(SXX, 6), middle])
    send(grads_in.at[:, middle], grads.at[:, middle])
    for end, x in enumerate((0, cx - 1)):
        for t in range(cy // ROWS):
            rows = pl.ds(t * ROWS, ROWS)
            both = strains(STEPS - 1, x, t)
            for index, value in enumerate(stresses(both, x, t)):
                s_end[index, end, rows, :] = value
            f = [fwd[index, x, rows, :] for index in range(6)]
            for index, value in enumerate(products(both, f)):
                g_end[index, end, rows, :] = grads_in[index, x, rows, :] + value
        send(s_end.at[:, end], out.at[pl.ds(SXX, 6), x])
        send(g_end.at[:, end], grads.at[:, x])
    for copy in copies:
        copy.wait()


def on_device(n_x, n_y, adjoint, buoyancy, lame_lambda, shear_mu, packed, scales, perm):
    fields, cx, cy, cz = adjoint.shape
    comp, segw = packed.shape[3:]
    lanes = min(128, segw)
    packed = packed.reshape(n_x, comp, segw // lanes, lanes)
    halos = 6 * STEPS
    pieces = PIECES if cy % (PIECES * ROWS) == 0 else 1
    dma = pltpu.SemaphoreType.DMA
    held = pl.pallas_call(
        functools.partial(kernel, n_x, n_y),
        out_shape=(pltpu.VMEM((fields, cx + 2, cy, cz), jnp.float32), pltpu.VMEM((3, cx, cy, cz), jnp.float32),
                   pltpu.VMEM((halos, cx, cz), jnp.float32), pltpu.VMEM((6, cx, cy, cz), jnp.float32),
                   pltpu.VMEM((2, cx, cy, cz), jnp.float32)),
        in_specs=[pl.BlockSpec(memory_space=pltpu.HBM)] * 7,
        out_specs=(pl.BlockSpec(memory_space=pltpu.VMEM),) * 5,
        scratch_shapes=[
            pltpu.VMEM((comp, cx, cy, cz), jnp.float32),
            pltpu.VMEM((halos, cx, cz), jnp.float32),
            pltpu.VMEM((STEPS, comp // STEPS, segw // lanes, lanes), jnp.int32),
            pltpu.VMEM((n_x, 1, comp), jnp.float32),
            pltpu.SMEM((n_x, 1, comp), jnp.float32),
            pltpu.SMEM(perm.shape, jnp.int32),
            pltpu.SMEM((n_x,), jnp.int32),
            dma((14,)), dma((STEPS,)), dma((STEPS,)), dma((halos, pieces)), dma((halos, pieces)), dma((halos,)), dma((halos,)),
            dma((n_x, STEPS)), dma((n_x, STEPS)), dma((n_x,)), dma((n_x,)), dma((3 + STEPS,)),
        ] + [pltpu.VMEM((n_x, comp // STEPS, segw // lanes, lanes), jnp.int32)] * STEPS,
        compiler_params=pltpu.CompilerParams(collective_id=0, has_side_effects=True,
                                             vmem_limit_bytes=VMEM_LIMIT),
    )(adjoint, buoyancy, lame_lambda, shear_mu, packed, scales, perm)
    return pl.pallas_call(
        finish,
        out_shape=(jax.ShapeDtypeStruct(adjoint.shape, jnp.float32), jax.ShapeDtypeStruct((2, cx, cy, cz), jnp.float32)),
        in_specs=[pl.BlockSpec(memory_space=pltpu.VMEM)] * 5,
        out_specs=(pl.BlockSpec(memory_space=pltpu.HBM),) * 2,
        scratch_shapes=[
            pltpu.VMEM((6, 2, cy, cz), jnp.float32),
            pltpu.VMEM((2, 2, cy, cz), jnp.float32),
            dma((9,)),
        ],
        compiler_params=pltpu.CompilerParams(vmem_limit_bytes=8000000),
    )(*held)


def solution(mesh):
    return jax.shard_map(
        functools.partial(on_device, mesh.shape["gx"], mesh.shape["gy"]),
        mesh=mesh,
        in_specs=(
            P(None, "gx", "gy", None),
            P("gx", "gy", None),
            P("gx", "gy", None),
            P("gx", "gy", None),
            P("gx", None, "gy", None, None),
            P("gx", None, "gy", None),
            P("gx", None),
        ),
        out_specs=(P(None, "gx", "gy", None), P(None, "gx", "gy", None)),
        check_vma=False,
    )
```

```python
import functools

import jax
import jax.numpy as jnp
from jax import lax
from jax.experimental import pallas as pl
from jax.experimental.pallas import tpu as pltpu
from jax.sharding import PartitionSpec as P

MESH = pl.DeviceIdType.MESH
STEPS = 2
COURANT = 0.15
ROWS = 8
PIECES = 2
VMEM_LIMIT = 60500000
TURN = 6
BENT = (((6, 0), (4, 0), (2, 0), (3, 0)), ((5, 0), (6, 1), (2, 1), (3, 1), (1, 0)), ((4, 1), (5, 1), (7, 0), (7, 1), (1, 1)), ())
STRAIGHT = (((4, 0), (6, 0), (2, 0)), ((5, 0), (3, 0), (7, 0), (1, 0), (0, 0)), ((4, 1), (5, 1), (2, 1), (3, 1), (6, 1), (7, 1), (1, 1)), ((0, 1),))

VX, VY, VZ, SXX, SYY, SZZ, SXY, SXZ, SYZ = range(9)

STRESS_X = ((0, (SXX,), -1), (1, (SXY, SXZ), 1))
STRESS_Y = ((0, (SYY,), -1), (1, (SXY, SYZ), 1))
SPEED_X = ((3, (VY, VZ), -1), (5, (VX,), 1))
SPEED_Y = ((3, (VX, VZ), -1), (5, (VY,), 1))


def partner(me, distance, count):
    if count & (count - 1):
        return lax.rem(me + distance, count)
    result, bit = me, 1
    while bit < count:
        if distance & bit:
            result = result + bit - 2 * bit * ((me // bit) % 2)
        bit *= 2
    return result


def stencil(cur, coef, halo_y):
    cx, cy, cz = coef.shape[1:]
    tiles = cy // ROWS
    sub = lax.broadcasted_iota(jnp.int32, (ROWS, cz), 0)
    lane = lax.broadcasted_iota(jnp.int32, (ROWS, cz), 1)
    first_row, last_row = sub == 0, sub == ROWS - 1
    first_lane, last_lane = lane == 0, lane == cz - 1

    def tile(field, x, t):
        return cur[field, x + 1, pl.ds(t * ROWS, ROWS), :]

    def z_before(value):
        return jnp.where(first_lane, 0.0, pltpu.roll(value, 1, 1))

    def z_after(value):
        return jnp.where(last_lane, 0.0, pltpu.roll(value, cz - 1, 1))

    def y_before(value, field, x, t, slot):
        row = halo_y[slot, pl.ds(x, 1), :] if t == 0 else cur[field, x + 1, pl.ds(t * ROWS - 1, 1), :]
        return jnp.where(first_row, jnp.broadcast_to(row, value.shape), pltpu.roll(value, 1, 0))

    def y_after(value, field, x, t, slot):
        row = halo_y[slot, pl.ds(x, 1), :] if t == tiles - 1 else cur[field, x + 1, pl.ds(t * ROWS + ROWS, 1), :]
        return jnp.where(last_row, jnp.broadcast_to(row, value.shape), pltpu.roll(value, ROWS - 1, 0))

    def strains(step, x, t):
        slot = 6 * step + 3
        vx, vy, vz = tile(VX, x, t), tile(VY, x, t), tile(VZ, x, t)
        exx = vx - tile(VX, x - 1, t)
        eyy = vy - y_before(vy, VY, x, t, slot + 2)
        ezz = vz - z_before(vz)
        exy = (y_after(vx, VX, x, t, slot) - vx) + (tile(VY, x + 1, t) - vy)
        exz = (z_after(vx) - vx) + (tile(VZ, x + 1, t) - vz)
        eyz = (z_after(vy) - vy) + (y_after(vz, VZ, x, t, slot + 1) - vz)
        return exx, eyy, ezz, exy, exz, eyz

    def stresses(both, x, t):
        rows = pl.ds(t * ROWS, ROWS)
        exx, eyy, ezz = both[:3]
        pull = (COURANT * coef[1, x, rows, :]) * (exx + eyy + ezz)
        mu = COURANT * coef[2, x, rows, :]
        moved = []
        for index, value in enumerate(both):
            change = pull + (2.0 * mu) * value if index < 3 else mu * value
            moved.append(tile(SXX + index, x, t) - change)
        return moved

    return tile, z_before, z_after, y_before, y_after, strains, stresses


def products(e, f):
    grad_lambda = (e[0] + e[1] + e[2]) * (f[0] + f[1] + f[2])
    grad_mu = 2.0 * (e[0] * f[0] + e[1] * f[1] + e[2] * f[2])
    return grad_lambda, grad_mu + e[3] * f[3] + e[4] * f[4] + e[5] * f[5]


def kernel(n_x, n_y, adj, buoy, lam, shear, packed, scales, perm_in, cur, coef, halo_y, fwd, grads,
           strain, send_y, relay, factors, factor_s, perm, inv,
           in_sem, rl_sem, rf_sem, xs_sem, xr_sem, ys_sem, yr_sem, ws_sem, wr_sem, fs_sem, fr_sem, loc_sem, *words):
    cx, cy, cz = buoy.shape
    comp = packed.shape[1]
    per_step = comp // STEPS
    lanes = packed.shape[3]
    segw = packed.shape[2] * lanes
    tiles = cy // ROWS
    pieces = xs_sem.shape[1]
    part = cy // pieces
    me_x, me_y = lax.axis_index("gx"), lax.axis_index("gy")

    loads = []

    def load(sem, source, target):
        copy = pltpu.make_async_copy(source, target, in_sem.at[sem])
        loads.append(copy)
        return copy

    edges = [load(12, adj.at[SXX, 0], cur.at[SXX, 1]),
             load(13, adj.at[pl.ds(SXY, 2), cx - 1], cur.at[pl.ds(SXY, 2), cx])]
    rows_in = [load(SYY, adj.at[SYY], cur.at[SYY, pl.ds(1, cx)]),
               load(SYZ, adj.at[SYZ], cur.at[SYZ, pl.ds(1, cx)]),
               load(SXY, adj.at[pl.ds(SXY, 2), pl.ds(0, cx - 1)], cur.at[pl.ds(SXY, 2), pl.ds(1, cx - 1)])]
    load(SXX, adj.at[SXX, pl.ds(1, cx - 1)], cur.at[SXX, pl.ds(2, cx - 1)])
    for index in (SZZ, VX, VY, VZ):
        load(index, adj.at[index], cur.at[index, pl.ds(1, cx)])
    for index, ref in enumerate((buoy, lam, shear)):
        load(9 + index, ref, coef.at[index])
    own_words = [pltpu.make_async_copy(packed.at[me_x, pl.ds(step * per_step, per_step)], words[step].at[me_x],
                                       loc_sem.at[2 + step]) for step in range(STEPS)]
    own_factor = pltpu.make_async_copy(scales.at[0, me_x], factors.at[me_x], loc_sem.at[1])
    for copy in loads[:len(edges)]:
        copy.start()

    barrier = pltpu.get_barrier_semaphore()
    for distance in range(1, n_x):
        pl.semaphore_signal(barrier, inc=1, device_id={"gx": partner(me_x, distance, n_x)}, device_id_type=MESH)

    def edge(way, axis):
        me, count = (me_x, n_x) if axis == "gx" else (me_y, n_y)
        return (me > 0) if way < 0 else (me < count - 1)

    for way in (-1, 1):
        @pl.when(edge(way, "gy"))
        def _():
            pl.semaphore_signal(barrier, inc=1, device_id={"gy": me_y + way}, device_id_type=MESH)

    for copy in loads[len(edges):]:
        copy.start()
    perm_copy = pltpu.make_async_copy(perm_in, perm, loc_sem.at[2 + STEPS])
    perm_copy.start()
    for copy in own_words:
        copy.start()
    own_factor.start()
    for way, place in ((-1, 0), (1, cx + 1)):
        @pl.when(jnp.logical_not(edge(way, "gx")))
        def _():
            for field in (VX, SXY, SXZ) if way < 0 else (VY, VZ, SXX):
                cur[field, place] = jnp.zeros((cy, cz), jnp.float32)

    pl.semaphore_wait(barrier, n_x - 1 + jnp.minimum(me_y, 1) + jnp.minimum(n_y - 1 - me_y, 1))

    def copy_x(step, message, piece):
        start, fields, way = message
        slot = 6 * step + start
        rows = pl.ds(piece * part, part)
        return pltpu.make_async_remote_copy(
            src_ref=cur.at[pl.ds(fields[0], len(fields)), 1 if way < 0 else cx, rows],
            dst_ref=cur.at[pl.ds(fields[0], len(fields)), cx + 1 if way < 0 else 0, rows],
            send_sem=xs_sem.at[slot, piece], recv_sem=xr_sem.at[slot, piece],
            device_id={"gx": me_x + way}, device_id_type=MESH)

    def copy_y(step, message):
        start, fields, way = message
        slot = 6 * step + start
        return pltpu.make_async_remote_copy(
            src_ref=send_y.at[pl.ds(slot, len(fields))], dst_ref=halo_y.at[pl.ds(slot, len(fields))],
            send_sem=ys_sem.at[slot], recv_sem=yr_sem.at[slot],
            device_id={"gy": me_y + way}, device_id_type=MESH)

    def word_copy(distance, step):
        to = partner(me_x, distance, n_x)
        stored = pl.ds(step * per_step, per_step)
        return pltpu.make_async_remote_copy(
            src_ref=packed.at[to, stored], dst_ref=words[step].at[me_x], send_sem=ws_sem.at[distance, step],
            recv_sem=wr_sem.at[distance, step], device_id={"gx": to}, device_id_type=MESH)

    def factor_copy(distance):
        to = partner(me_x, distance, n_x)
        return pltpu.make_async_remote_copy(
            src_ref=scales.at[0, to], dst_ref=factors.at[me_x], send_sem=fs_sem.at[distance],
            recv_sem=fr_sem.at[distance], device_id={"gx": to}, device_id_type=MESH)

    def send_x(step, messages, piece):
        for message in messages:
            @pl.when(edge(message[2], "gx"))
            def _():
                copy_x(step, message, piece).start()

    def send_rows(step, messages, toward):
        for message in messages:
            start, fields, way = message
            if way != toward:
                continue

            @pl.when(edge(way, "gy"))
            def _():
                row = 0 if way < 0 else cy - 1
                for offset, field in enumerate(fields):
                    for x in range(cx):
                        send_y[6 * step + start + offset, pl.ds(x, 1), :] = cur[field, 1 + x, pl.ds(row, 1), :]
                copy_y(step, message).start()

    def finish_sends(step, messages_x, messages_y):
        for message in messages_x:
            @pl.when(edge(message[2], "gx"))
            def _():
                for piece in range(pieces):
                    copy_x(step, message, piece).wait_send()
        for message in messages_y:
            @pl.when(edge(message[2], "gy"))
            def _():
                copy_y(step, message).wait_send()

    def receive_y(step, messages, toward):
        for message in messages:
            start, fields, way = message
            if way != toward:
                continue

            @pl.when(edge(-way, "gy"))
            def _():
                copy_y(step, message).wait_recv()

            @pl.when(jnp.logical_not(edge(-way, "gy")))
            def _():
                for offset in range(len(fields)):
                    halo_y[6 * step + start + offset] = jnp.zeros((cx, cz), jnp.float32)

    def receive_x(step, messages, piece):
        for message in messages:
            @pl.when(edge(-message[2], "gx"))
            def _():
                copy_x(step, message, piece).wait_recv()

    relays = n_x > TURN and n_x & (n_x - 1) == 0
    bent = (me_x // (TURN & -TURN)) % 2 != (me_x // (TURN - (TURN & -TURN))) % 2
    low, high = TURN & -TURN, TURN - (TURN & -TURN)

    def first_leg(step):
        return pltpu.make_async_remote_copy(
            src_ref=packed.at[partner(me_x, TURN, n_x), pl.ds(step * per_step, per_step)], dst_ref=relay.at[step],
            send_sem=ws_sem.at[TURN, step], recv_sem=rl_sem.at[step],
            device_id={"gx": partner(me_x, high, n_x)}, device_id_type=MESH)

    def second_leg(step):
        return pltpu.make_async_remote_copy(
            src_ref=relay.at[step], dst_ref=words[step].at[partner(me_x, high, n_x)],
            send_sem=rf_sem.at[step], recv_sem=wr_sem.at[TURN, step],
            device_id={"gx": partner(me_x, low, n_x)}, device_id_type=MESH)

    def send_words(table, turned):
        for kind, step in table:
            if kind == 0 and relays:
                first_leg(step).wait_recv()
                second_leg(step).start()
            for distance in range(1, n_x):
                if max(distance * 8 // n_x, 1) == kind:
                    if turned and distance == TURN:
                        first_leg(step).start()
                    else:
                        word_copy(distance, step).start()

    def send_group(which):
        if relays:
            @pl.when(bent)
            def _():
                send_words(BENT[which], True)

            @pl.when(jnp.logical_not(bent))
            def _():
                send_words(STRAIGHT[which], False)
        else:
            send_words(STRAIGHT[which], False)
        if which == 0:
            for distance in range(1, n_x):
                factor_copy(distance).start()

    def receive_words(step):
        if step == 0:
            own_factor.wait()
            for distance in range(1, n_x):
                factor_copy(distance).wait()
            to_scalar = pltpu.make_async_copy(factors, factor_s, loc_sem.at[0])
            to_scalar.start()
            to_scalar.wait()
        own_words[step].wait()
        for distance in range(1, n_x):
            word_copy(distance, step).wait()
        if relays:
            @pl.when(jnp.logical_not(bent))
            def _():
                second_leg(step).wait_send()

    tile, z_before, z_after, y_before, y_after, strains, stresses = stencil(cur, coef, halo_y)

    def velocity(step, which, x):
        slot = 6 * step
        for t in which:
            rows = pl.ds(t * ROWS, ROWS)
            scaled = COURANT * coef[0, x, rows, :]
            sxy, sxz, syz = tile(SXY, x, t), tile(SXZ, x, t), tile(SYZ, x, t)
            sxx, syy, szz = tile(SXX, x, t), tile(SYY, x, t), tile(SZZ, x, t)
            moved = (
                tile(VX, x, t) - scaled * (
                    (tile(SXX, x + 1, t) - sxx) + (sxy - y_before(sxy, SXY, x, t, slot + 1)) + (sxz - z_before(sxz))),
                tile(VY, x, t) - scaled * (
                    (sxy - tile(SXY, x - 1, t)) + (y_after(syy, SYY, x, t, slot) - syy) + (syz - z_before(syz))),
                tile(VZ, x, t) - scaled * (
                    (sxz - tile(SXZ, x - 1, t)) + (syz - y_before(syz, SYZ, x, t, slot + 2)) + (z_after(szz) - szz)))
            for field, value in enumerate(moved):
                cur[field, x + 1, rows, :] = value

    def stress(step, which, x):
        for t in which:
            rows = pl.ds(t * ROWS, ROWS)
            both = strains(step, x, t)
            for index, value in enumerate(both):
                strain[6 * step + index, x, rows, :] = value
            for index, value in enumerate(stresses(both, x, t)):
                cur[SXX + index, x + 1, rows, :] = value

    def over(first, last, body):
        def run(x, carry):
            body(x)
            return carry
        lax.fori_loop(first, last, run, 0)

    def ends(body):
        def run(index, carry):
            body(index * (cx - 1))
            return carry
        lax.fori_loop(0, 2, run, 0)

    width = lanes
    per_x = cy * cz // (4 * segw)

    def source(row, chunk):
        offset = row * cz + chunk * width
        within = offset % (4 * segw)
        return offset // (4 * segw), within % segw, within // segw

    sub_w = lax.broadcasted_iota(jnp.int32, (ROWS, width), 0)

    def gradient(step, keep, x):
        made = {}
        for t in range(tiles):
            for chunk in range(cz // width):
                rows = pl.ds(t * ROWS, ROWS)
                columns = pl.ds(chunk * width, width)
                plan = [source(t * ROWS + r, chunk) for r in range(ROWS)]
                shift = jnp.full((ROWS, width), 8 * plan[0][2], jnp.int32)
                for r in range(1, ROWS):
                    if plan[r][2] != plan[r - 1][2]:
                        shift = jnp.where(sub_w >= r, 8 * plan[r][2], shift)
                key = tuple(p[:2] for p in plan)
                distinct = list(dict.fromkeys(key))
                masks = []
                for item in distinct[1:]:
                    mask = None
                    for r in range(ROWS):
                        if key[r] == item:
                            mask = (sub_w == r) if mask is None else mask | (sub_w == r)
                    masks.append(mask)
                holders = {b: inv[x * per_x + b] for b in dict.fromkeys(k[0] for k in key)}
                blocks = [k[0] for k in key]

                def stored(c):
                    if (key, c) not in made:
                        word = None
                        for position, (block, start) in enumerate(distinct):
                            piece = jnp.broadcast_to(
                                words[step][holders[block], c - per_step * step, pl.ds(start // lanes, 1), :], (ROWS, width))
                            word = piece if word is None else jnp.where(masks[position - 1], piece, word)
                        made[key, c] = word ^ jnp.int32(-2147483648)
                    byte = (lax.shift_right_logical(made[key, c], shift) & 255) - 128
                    factor = None
                    for r in range(ROWS):
                        if r == 0:
                            factor = factor_s[holders[blocks[0]], 0, c]
                        elif blocks[r] != blocks[r - 1]:
                            factor = jnp.where(sub_w >= r, factor_s[holders[blocks[r]], 0, c], factor)
                    return byte.astype(jnp.float32) * factor

                f = [stored(6 * step + index) for index in range(6)]
                if keep:
                    for index, value in enumerate(f):
                        fwd[index, x, rows, columns] = value
                else:
                    e = [strain[6 * step + index, x, rows, columns] for index in range(6)]
                    grad_lambda, grad_mu = products(e, f)
                    if step > 0:
                        grad_lambda = grads[0, x, rows, columns] + grad_lambda
                        grad_mu = grads[1, x, rows, columns] + grad_mu
                    grads[0, x, rows, columns] = grad_lambda
                    grads[1, x, rows, columns] = grad_mu

    def inside(piece):
        return range(piece * part // ROWS, (piece + 1) * part // ROWS)

    outer = (0, tiles - 1) if tiles > 1 else (0,)
    inner = range(1, tiles - 1)
    def phase(step, body, taken, taken_y, given_step, given, given_y, group):
        over(1, cx - 1, functools.partial(body, step, inner))
        for piece in range(pieces):
            rim = [t for t in inside(piece) if t in outer]
            for t, way in ((0, 1), (tiles - 1, -1)):
                if t in inside(piece):
                    receive_y(step, taken_y, way)
            if rim:
                over(1, cx - 1, functools.partial(body, step, rim))
            receive_x(step, taken, piece)
            ends(functools.partial(body, step, inside(piece)))
            send_x(given_step, given, piece)
            for t, way in ((0, -1), (tiles - 1, 1)):
                if t in inside(piece):
                    send_rows(given_step, given_y, way)
        send_group(group)

    for copy in edges:
        copy.wait()
    for piece in range(pieces):
        send_x(0, STRESS_X, piece)
    for copy in rows_in:
        copy.wait()
    for way in (-1, 1):
        send_rows(0, STRESS_Y, way)
    send_group(0)
    perm_copy.wait()

    def invert(block, carry):
        total = jnp.int32(0)
        for holder in range(n_x):
            total = jnp.where(perm[0, holder] == block, holder, total)
        inv[block] = total
        return carry
    lax.fori_loop(0, n_x, invert, 0)
    for copy in loads[len(edges) + len(rows_in):]:
        copy.wait()

    final = STEPS - 1
    for step in range(STEPS):
        if step > 0:
            finish_sends(step - 1, SPEED_X, SPEED_Y)
        phase(step, velocity, STRESS_X, STRESS_Y, step, SPEED_X, SPEED_Y, 1 + 2 * step)
        if step > 0:
            receive_words(step - 1)
            over(0, cx, functools.partial(gradient, step - 1, False))
        finish_sends(step, STRESS_X, STRESS_Y)
        if step < final:
            phase(step, stress, SPEED_X, SPEED_Y, step + 1, STRESS_X, STRESS_Y, 2 + 2 * step)
    over(1, cx - 1, functools.partial(stress, final, inner))
    for way in (1, -1):
        receive_y(final, SPEED_Y, way)
    over(1, cx - 1, functools.partial(stress, final, outer))
    receive_words(final)
    over(1, cx - 1, functools.partial(gradient, final, False))
    ends(functools.partial(gradient, final, True))
    for piece in range(pieces):
        receive_x(final, SPEED_X, piece)
    finish_sends(final, SPEED_X, SPEED_Y)


def finish(cur, coef, halo_y, fwd, grads_in, out, grads, s_end, g_end, sem):
    cx, cy, cz = coef.shape[1:]
    tile, z_before, z_after, y_before, y_after, strains, stresses = stencil(cur, coef, halo_y)
    copies = []

    def send(source, target):
        copies.append(pltpu.make_async_copy(source, target, sem.at[len(copies)]))
        copies[-1].start()

    for field in (VX, VY, VZ):
        send(cur.at[field, pl.ds(1, cx)], out.at[field])
    middle = pl.ds(1, cx - 2)
    send(cur.at[pl.ds(SXX, 6), pl.ds(2, cx - 2)], out.at[pl.ds(SXX, 6), middle])
    send(grads_in.at[:, middle], grads.at[:, middle])
    for end, x in enumerate((0, cx - 1)):
        for t in range(cy // ROWS):
            rows = pl.ds(t * ROWS, ROWS)
            both = strains(STEPS - 1, x, t)
            for index, value in enumerate(stresses(both, x, t)):
                s_end[index, end, rows, :] = value
            f = [fwd[index, x, rows, :] for index in range(6)]
            for index, value in enumerate(products(both, f)):
                g_end[index, end, rows, :] = grads_in[index, x, rows, :] + value
        send(s_end.at[:, end], out.at[pl.ds(SXX, 6), x])
        send(g_end.at[:, end], grads.at[:, x])
    for copy in copies:
        copy.wait()


def on_device(n_x, n_y, adjoint, buoyancy, lame_lambda, shear_mu, packed, scales, perm):
    fields, cx, cy, cz = adjoint.shape
    comp, segw = packed.shape[3:]
    lanes = min(128, segw)
    packed = packed.reshape(n_x, comp, segw // lanes, lanes)
    halos = 6 * STEPS
    pieces = PIECES if cy % (PIECES * ROWS) == 0 else 1
    dma = pltpu.SemaphoreType.DMA
    held = pl.pallas_call(
        functools.partial(kernel, n_x, n_y),
        out_shape=(pltpu.VMEM((fields, cx + 2, cy, cz), jnp.float32), pltpu.VMEM((3, cx, cy, cz), jnp.float32),
                   pltpu.VMEM((halos, cx, cz), jnp.float32), pltpu.VMEM((6, cx, cy, cz), jnp.float32),
                   pltpu.VMEM((2, cx, cy, cz), jnp.float32)),
        in_specs=[pl.BlockSpec(memory_space=pltpu.HBM)] * 7,
        out_specs=(pl.BlockSpec(memory_space=pltpu.VMEM),) * 5,
        scratch_shapes=[
            pltpu.VMEM((comp, cx, cy, cz), jnp.float32),
            pltpu.VMEM((halos, cx, cz), jnp.float32),
            pltpu.VMEM((STEPS, comp // STEPS, segw // lanes, lanes), jnp.int32),
            pltpu.VMEM((n_x, 1, comp), jnp.float32),
            pltpu.SMEM((n_x, 1, comp), jnp.float32),
            pltpu.SMEM(perm.shape, jnp.int32),
            pltpu.SMEM((n_x,), jnp.int32),
            dma((14,)), dma((STEPS,)), dma((STEPS,)), dma((halos, pieces)), dma((halos, pieces)), dma((halos,)), dma((halos,)),
            dma((n_x, STEPS)), dma((n_x, STEPS)), dma((n_x,)), dma((n_x,)), dma((3 + STEPS,)),
        ] + [pltpu.VMEM((n_x, comp // STEPS, segw // lanes, lanes), jnp.int32)] * STEPS,
        compiler_params=pltpu.CompilerParams(collective_id=0, has_side_effects=True,
                                             vmem_limit_bytes=VMEM_LIMIT),
    )(adjoint, buoyancy, lame_lambda, shear_mu, packed, scales, perm)
    return pl.pallas_call(
        finish,
        out_shape=(jax.ShapeDtypeStruct(adjoint.shape, jnp.float32), jax.ShapeDtypeStruct((2, cx, cy, cz), jnp.float32)),
        in_specs=[pl.BlockSpec(memory_space=pltpu.VMEM)] * 5,
        out_specs=(pl.BlockSpec(memory_space=pltpu.HBM),) * 2,
        scratch_shapes=[
            pltpu.VMEM((6, 2, cy, cz), jnp.float32),
            pltpu.VMEM((2, 2, cy, cz), jnp.float32),
            dma((9,)),
        ],
        compiler_params=pltpu.CompilerParams(vmem_limit_bytes=8000000),
    )(*held)


def solution(mesh):
    return jax.shard_map(
        functools.partial(on_device, mesh.shape["gx"], mesh.shape["gy"]),
        mesh=mesh,
        in_specs=(
            P(None, "gx", "gy", None),
            P("gx", "gy", None),
            P("gx", "gy", None),
            P("gx", "gy", None),
            P("gx", None, "gy", None, None),
            P("gx", None, "gy", None),
            P("gx", None),
        ),
        out_specs=(P(None, "gx", "gy", None), P(None, "gx", "gy", None)),
        check_vma=False,
    )
```

```python
import functools

import jax
import jax.numpy as jnp
from jax import lax
from jax.experimental import pallas as pl
from jax.experimental.pallas import tpu as pltpu
from jax.sharding import PartitionSpec as P

MESH = pl.DeviceIdType.MESH
STEPS = 2
COURANT = 0.15
ROWS = 8
PIECES = 2
VMEM_LIMIT = 60500000
TURN = 6
RELAYED = ((6, 0), (6, 1))
BENT = (((6, 0), (6, 1), (2, 0), (3, 0)), ((4, 0), (5, 0), (2, 1), (3, 1), (1, 0)), ((4, 1), (5, 1), (7, 0), (7, 1), (1, 1)), ())
STRAIGHT = (((6, 0), (2, 0)), ((4, 0), (5, 0), (3, 0), (7, 0), (1, 0), (0, 0)), ((4, 1), (5, 1), (2, 1), (3, 1), (6, 1), (7, 1), (1, 1), (0, 1)), ())

VX, VY, VZ, SXX, SYY, SZZ, SXY, SXZ, SYZ = range(9)

STRESS_X = ((0, (SXX,), -1), (1, (SXY, SXZ), 1))
STRESS_Y = ((0, (SYY,), -1), (1, (SXY, SYZ), 1))
SPEED_X = ((3, (VY, VZ), -1), (5, (VX,), 1))
SPEED_Y = ((3, (VX, VZ), -1), (5, (VY,), 1))


def partner(me, distance, count):
    if count & (count - 1):
        return lax.rem(me + distance, count)
    result, bit = me, 1
    while bit < count:
        if distance & bit:
            result = result + bit - 2 * bit * ((me // bit) % 2)
        bit *= 2
    return result


def stencil(cur, coef, halo_y):
    cx, cy, cz = coef.shape[1:]
    tiles = cy // ROWS
    sub = lax.broadcasted_iota(jnp.int32, (ROWS, cz), 0)
    lane = lax.broadcasted_iota(jnp.int32, (ROWS, cz), 1)
    first_row, last_row = sub == 0, sub == ROWS - 1
    first_lane, last_lane = lane == 0, lane == cz - 1

    def tile(field, x, t):
        return cur[field, x + 1, pl.ds(t * ROWS, ROWS), :]

    def z_before(value):
        return jnp.where(first_lane, 0.0, pltpu.roll(value, 1, 1))

    def z_after(value):
        return jnp.where(last_lane, 0.0, pltpu.roll(value, cz - 1, 1))

    def y_before(value, field, x, t, slot):
        row = halo_y[slot, pl.ds(x, 1), :] if t == 0 else cur[field, x + 1, pl.ds(t * ROWS - 1, 1), :]
        return jnp.where(first_row, jnp.broadcast_to(row, value.shape), pltpu.roll(value, 1, 0))

    def y_after(value, field, x, t, slot):
        row = halo_y[slot, pl.ds(x, 1), :] if t == tiles - 1 else cur[field, x + 1, pl.ds(t * ROWS + ROWS, 1), :]
        return jnp.where(last_row, jnp.broadcast_to(row, value.shape), pltpu.roll(value, ROWS - 1, 0))

    def strains(step, x, t):
        slot = 6 * step + 3
        vx, vy, vz = tile(VX, x, t), tile(VY, x, t), tile(VZ, x, t)
        exx = vx - tile(VX, x - 1, t)
        eyy = vy - y_before(vy, VY, x, t, slot + 2)
        ezz = vz - z_before(vz)
        exy = (y_after(vx, VX, x, t, slot) - vx) + (tile(VY, x + 1, t) - vy)
        exz = (z_after(vx) - vx) + (tile(VZ, x + 1, t) - vz)
        eyz = (z_after(vy) - vy) + (y_after(vz, VZ, x, t, slot + 1) - vz)
        return exx, eyy, ezz, exy, exz, eyz

    def stresses(both, x, t):
        rows = pl.ds(t * ROWS, ROWS)
        exx, eyy, ezz = both[:3]
        pull = (COURANT * coef[1, x, rows, :]) * (exx + eyy + ezz)
        mu = COURANT * coef[2, x, rows, :]
        moved = []
        for index, value in enumerate(both):
            change = pull + (2.0 * mu) * value if index < 3 else mu * value
            moved.append(tile(SXX + index, x, t) - change)
        return moved

    return tile, z_before, z_after, y_before, y_after, strains, stresses


def products(e, f):
    grad_lambda = (e[0] + e[1] + e[2]) * (f[0] + f[1] + f[2])
    grad_mu = 2.0 * (e[0] * f[0] + e[1] * f[1] + e[2] * f[2])
    return grad_lambda, grad_mu + e[3] * f[3] + e[4] * f[4] + e[5] * f[5]


def kernel(n_x, n_y, adj, buoy, lam, shear, packed, scales, perm_in, cur, coef, halo_y, fwd, grads,
           strain, send_y, relay, factors, factor_s, perm, inv,
           in_sem, rl_sem, rf_sem, xs_sem, xr_sem, ys_sem, yr_sem, ws_sem, wr_sem, fs_sem, fr_sem, loc_sem, *words):
    cx, cy, cz = buoy.shape
    comp = packed.shape[1]
    per_step = comp // STEPS
    lanes = packed.shape[3]
    segw = packed.shape[2] * lanes
    tiles = cy // ROWS
    pieces = xs_sem.shape[1]
    part = cy // pieces
    me_x, me_y = lax.axis_index("gx"), lax.axis_index("gy")

    loads = []

    def load(sem, source, target):
        copy = pltpu.make_async_copy(source, target, in_sem.at[sem])
        loads.append(copy)
        return copy

    edges = [load(12, adj.at[SXX, 0], cur.at[SXX, 1]),
             load(13, adj.at[pl.ds(SXY, 2), cx - 1], cur.at[pl.ds(SXY, 2), cx])]
    rows_in = [load(SYY, adj.at[SYY], cur.at[SYY, pl.ds(1, cx)]),
               load(SYZ, adj.at[SYZ], cur.at[SYZ, pl.ds(1, cx)]),
               load(SXY, adj.at[pl.ds(SXY, 2), pl.ds(0, cx - 1)], cur.at[pl.ds(SXY, 2), pl.ds(1, cx - 1)])]
    load(SXX, adj.at[SXX, pl.ds(1, cx - 1)], cur.at[SXX, pl.ds(2, cx - 1)])
    for index in (SZZ, VX, VY, VZ):
        load(index, adj.at[index], cur.at[index, pl.ds(1, cx)])
    for index, ref in enumerate((buoy, lam, shear)):
        load(9 + index, ref, coef.at[index])
    own_words = [pltpu.make_async_copy(packed.at[me_x, pl.ds(step * per_step, per_step)], words[step].at[me_x],
                                       loc_sem.at[2 + step]) for step in range(STEPS)]
    own_factor = pltpu.make_async_copy(scales.at[0, me_x], factors.at[me_x], loc_sem.at[1])
    for copy in loads[:len(edges)]:
        copy.start()

    barrier = pltpu.get_barrier_semaphore()
    for distance in range(1, n_x):
        pl.semaphore_signal(barrier, inc=1, device_id={"gx": partner(me_x, distance, n_x)}, device_id_type=MESH)

    def edge(way, axis):
        me, count = (me_x, n_x) if axis == "gx" else (me_y, n_y)
        return (me > 0) if way < 0 else (me < count - 1)

    for way in (-1, 1):
        @pl.when(edge(way, "gy"))
        def _():
            pl.semaphore_signal(barrier, inc=1, device_id={"gy": me_y + way}, device_id_type=MESH)

    for copy in loads[len(edges):]:
        copy.start()
    perm_copy = pltpu.make_async_copy(perm_in, perm, loc_sem.at[2 + STEPS])
    perm_copy.start()
    for copy in own_words:
        copy.start()
    own_factor.start()
    for way, place in ((-1, 0), (1, cx + 1)):
        @pl.when(jnp.logical_not(edge(way, "gx")))
        def _():
            for field in (VX, SXY, SXZ) if way < 0 else (VY, VZ, SXX):
                cur[field, place] = jnp.zeros((cy, cz), jnp.float32)

    pl.semaphore_wait(barrier, n_x - 1 + jnp.minimum(me_y, 1) + jnp.minimum(n_y - 1 - me_y, 1))

    def copy_x(step, message, piece):
        start, fields, way = message
        slot = 6 * step + start
        rows = pl.ds(piece * part, part)
        return pltpu.make_async_remote_copy(
            src_ref=cur.at[pl.ds(fields[0], len(fields)), 1 if way < 0 else cx, rows],
            dst_ref=cur.at[pl.ds(fields[0], len(fields)), cx + 1 if way < 0 else 0, rows],
            send_sem=xs_sem.at[slot, piece], recv_sem=xr_sem.at[slot, piece],
            device_id={"gx": me_x + way}, device_id_type=MESH)

    def copy_y(step, message):
        start, fields, way = message
        slot = 6 * step + start
        return pltpu.make_async_remote_copy(
            src_ref=send_y.at[pl.ds(slot, len(fields))], dst_ref=halo_y.at[pl.ds(slot, len(fields))],
            send_sem=ys_sem.at[slot], recv_sem=yr_sem.at[slot],
            device_id={"gy": me_y + way}, device_id_type=MESH)

    def word_copy(distance, step):
        to = partner(me_x, distance, n_x)
        stored = pl.ds(step * per_step, per_step)
        return pltpu.make_async_remote_copy(
            src_ref=packed.at[to, stored], dst_ref=words[step].at[me_x], send_sem=ws_sem.at[distance, step],
            recv_sem=wr_sem.at[distance, step], device_id={"gx": to}, device_id_type=MESH)

    def factor_copy(distance):
        to = partner(me_x, distance, n_x)
        return pltpu.make_async_remote_copy(
            src_ref=scales.at[0, to], dst_ref=factors.at[me_x], send_sem=fs_sem.at[distance],
            recv_sem=fr_sem.at[distance], device_id={"gx": to}, device_id_type=MESH)

    def send_x(step, messages, piece):
        for message in messages:
            @pl.when(edge(message[2], "gx"))
            def _():
                copy_x(step, message, piece).start()

    def send_rows(step, messages, toward):
        for message in messages:
            start, fields, way = message
            if way != toward:
                continue

            @pl.when(edge(way, "gy"))
            def _():
                row = 0 if way < 0 else cy - 1
                for offset, field in enumerate(fields):
                    for x in range(cx):
                        send_y[6 * step + start + offset, pl.ds(x, 1), :] = cur[field, 1 + x, pl.ds(row, 1), :]
                copy_y(step, message).start()

    def finish_sends(step, messages_x, messages_y):
        for message in messages_x:
            @pl.when(edge(message[2], "gx"))
            def _():
                for piece in range(pieces):
                    copy_x(step, message, piece).wait_send()
        for message in messages_y:
            @pl.when(edge(message[2], "gy"))
            def _():
                copy_y(step, message).wait_send()

    def receive_y(step, messages, toward):
        for message in messages:
            start, fields, way = message
            if way != toward:
                continue

            @pl.when(edge(-way, "gy"))
            def _():
                copy_y(step, message).wait_recv()

            @pl.when(jnp.logical_not(edge(-way, "gy")))
            def _():
                for offset in range(len(fields)):
                    halo_y[6 * step + start + offset] = jnp.zeros((cx, cz), jnp.float32)

    def receive_x(step, messages, piece):
        for message in messages:
            @pl.when(edge(-message[2], "gx"))
            def _():
                copy_x(step, message, piece).wait_recv()

    relays = n_x > max(distance for distance, _ in RELAYED) and n_x & (n_x - 1) == 0
    bent = (me_x // (TURN & -TURN)) % 2 != (me_x // (TURN - (TURN & -TURN))) % 2
    low, high = TURN & -TURN, TURN - (TURN & -TURN)

    def first_leg(index):
        distance, step = RELAYED[index]
        return pltpu.make_async_remote_copy(
            src_ref=packed.at[partner(me_x, distance, n_x), pl.ds(step * per_step, per_step)], dst_ref=relay.at[index],
            send_sem=ws_sem.at[distance, step], recv_sem=rl_sem.at[index],
            device_id={"gx": partner(me_x, high, n_x)}, device_id_type=MESH)

    def second_leg(index):
        distance, step = RELAYED[index]
        return pltpu.make_async_remote_copy(
            src_ref=relay.at[index], dst_ref=words[step].at[partner(me_x, high, n_x)],
            send_sem=rf_sem.at[index], recv_sem=wr_sem.at[distance, step],
            device_id={"gx": partner(me_x, distance - high, n_x)}, device_id_type=MESH)

    def send_words(table, turned):
        for kind, step in table:
            if kind == 0 and relays:
                first_leg(step).wait_recv()
                second_leg(step).start()
                continue
            for distance in range(1, n_x):
                if max(distance * 8 // n_x, 1) == kind:
                    if turned and (distance, step) in RELAYED:
                        first_leg(RELAYED.index((distance, step))).start()
                    else:
                        word_copy(distance, step).start()

    def send_group(which):
        if relays:
            @pl.when(bent)
            def _():
                send_words(BENT[which], True)

            @pl.when(jnp.logical_not(bent))
            def _():
                send_words(STRAIGHT[which], False)
        else:
            send_words(STRAIGHT[which], False)
        if which == 0:
            for distance in range(1, n_x):
                factor_copy(distance).start()

    def receive_words(step):
        if step == 0:
            own_factor.wait()
            for distance in range(1, n_x):
                factor_copy(distance).wait()
            to_scalar = pltpu.make_async_copy(factors, factor_s, loc_sem.at[0])
            to_scalar.start()
            to_scalar.wait()
        own_words[step].wait()
        for distance in range(1, n_x):
            word_copy(distance, step).wait()
        if relays:
            @pl.when(jnp.logical_not(bent))
            def _():
                for index, (_, told) in enumerate(RELAYED):
                    if told == step:
                        second_leg(index).wait_send()

    tile, z_before, z_after, y_before, y_after, strains, stresses = stencil(cur, coef, halo_y)

    def velocity(step, which, x):
        slot = 6 * step
        for t in which:
            rows = pl.ds(t * ROWS, ROWS)
            scaled = COURANT * coef[0, x, rows, :]
            sxy, sxz, syz = tile(SXY, x, t), tile(SXZ, x, t), tile(SYZ, x, t)
            sxx, syy, szz = tile(SXX, x, t), tile(SYY, x, t), tile(SZZ, x, t)
            moved = (
                tile(VX, x, t) - scaled * (
                    (tile(SXX, x + 1, t) - sxx) + (sxy - y_before(sxy, SXY, x, t, slot + 1)) + (sxz - z_before(sxz))),
                tile(VY, x, t) - scaled * (
                    (sxy - tile(SXY, x - 1, t)) + (y_after(syy, SYY, x, t, slot) - syy) + (syz - z_before(syz))),
                tile(VZ, x, t) - scaled * (
                    (sxz - tile(SXZ, x - 1, t)) + (syz - y_before(syz, SYZ, x, t, slot + 2)) + (z_after(szz) - szz)))
            for field, value in enumerate(moved):
                cur[field, x + 1, rows, :] = value

    def stress(step, which, x):
        for t in which:
            rows = pl.ds(t * ROWS, ROWS)
            both = strains(step, x, t)
            for index, value in enumerate(both):
                strain[6 * step + index, x, rows, :] = value
            for index, value in enumerate(stresses(both, x, t)):
                cur[SXX + index, x + 1, rows, :] = value

    def over(first, last, body):
        def run(x, carry):
            body(x)
            return carry
        lax.fori_loop(first, last, run, 0)

    def ends(body):
        def run(index, carry):
            body(index * (cx - 1))
            return carry
        lax.fori_loop(0, 2, run, 0)

    width = lanes
    per_x = cy * cz // (4 * segw)

    def source(row, chunk):
        offset = row * cz + chunk * width
        within = offset % (4 * segw)
        return offset // (4 * segw), within % segw, within // segw

    sub_w = lax.broadcasted_iota(jnp.int32, (ROWS, width), 0)

    def gradient(step, keep, x):
        made = {}
        for t in range(tiles):
            for chunk in range(cz // width):
                rows = pl.ds(t * ROWS, ROWS)
                columns = pl.ds(chunk * width, width)
                plan = [source(t * ROWS + r, chunk) for r in range(ROWS)]
                shift = jnp.full((ROWS, width), 8 * plan[0][2], jnp.int32)
                for r in range(1, ROWS):
                    if plan[r][2] != plan[r - 1][2]:
                        shift = jnp.where(sub_w >= r, 8 * plan[r][2], shift)
                key = tuple(p[:2] for p in plan)
                distinct = list(dict.fromkeys(key))
                masks = []
                for item in distinct[1:]:
                    mask = None
                    for r in range(ROWS):
                        if key[r] == item:
                            mask = (sub_w == r) if mask is None else mask | (sub_w == r)
                    masks.append(mask)
                holders = {b: inv[x * per_x + b] for b in dict.fromkeys(k[0] for k in key)}
                blocks = [k[0] for k in key]

                def stored(c):
                    if (key, c) not in made:
                        word = None
                        for position, (block, start) in enumerate(distinct):
                            piece = jnp.broadcast_to(
                                words[step][holders[block], c - per_step * step, pl.ds(start // lanes, 1), :], (ROWS, width))
                            word = piece if word is None else jnp.where(masks[position - 1], piece, word)
                        made[key, c] = word ^ jnp.int32(-2147483648)
                    byte = (lax.shift_right_logical(made[key, c], shift) & 255) - 128
                    factor = None
                    for r in range(ROWS):
                        if r == 0:
                            factor = factor_s[holders[blocks[0]], 0, c]
                        elif blocks[r] != blocks[r - 1]:
                            factor = jnp.where(sub_w >= r, factor_s[holders[blocks[r]], 0, c], factor)
                    return byte.astype(jnp.float32) * factor

                f = [stored(6 * step + index) for index in range(6)]
                if keep:
                    for index, value in enumerate(f):
                        fwd[index, x, rows, columns] = value
                else:
                    e = [strain[6 * step + index, x, rows, columns] for index in range(6)]
                    grad_lambda, grad_mu = products(e, f)
                    if step > 0:
                        grad_lambda = grads[0, x, rows, columns] + grad_lambda
                        grad_mu = grads[1, x, rows, columns] + grad_mu
                    grads[0, x, rows, columns] = grad_lambda
                    grads[1, x, rows, columns] = grad_mu

    def inside(piece):
        return range(piece * part // ROWS, (piece + 1) * part // ROWS)

    outer = (0, tiles - 1) if tiles > 1 else (0,)
    inner = range(1, tiles - 1)
    def phase(step, body, taken, taken_y, given_step, given, given_y, group):
        over(1, cx - 1, functools.partial(body, step, inner))
        for piece in range(pieces):
            rim = [t for t in inside(piece) if t in outer]
            for t, way in ((0, 1), (tiles - 1, -1)):
                if t in inside(piece):
                    receive_y(step, taken_y, way)
            if rim:
                over(1, cx - 1, functools.partial(body, step, rim))
            receive_x(step, taken, piece)
            ends(functools.partial(body, step, inside(piece)))
            send_x(given_step, given, piece)
            for t, way in ((0, -1), (tiles - 1, 1)):
                if t in inside(piece):
                    send_rows(given_step, given_y, way)
        send_group(group)

    for copy in edges:
        copy.wait()
    for piece in range(pieces):
        send_x(0, STRESS_X, piece)
    for copy in rows_in:
        copy.wait()
    for way in (-1, 1):
        send_rows(0, STRESS_Y, way)
    send_group(0)
    perm_copy.wait()

    def invert(block, carry):
        total = jnp.int32(0)
        for holder in range(n_x):
            total = jnp.where(perm[0, holder] == block, holder, total)
        inv[block] = total
        return carry
    lax.fori_loop(0, n_x, invert, 0)
    for copy in loads[len(edges) + len(rows_in):]:
        copy.wait()

    final = STEPS - 1
    for step in range(STEPS):
        if step > 0:
            finish_sends(step - 1, SPEED_X, SPEED_Y)
        phase(step, velocity, STRESS_X, STRESS_Y, step, SPEED_X, SPEED_Y, 1 + 2 * step)
        if step > 0:
            receive_words(step - 1)
            over(0, cx, functools.partial(gradient, step - 1, False))
        finish_sends(step, STRESS_X, STRESS_Y)
        if step < final:
            phase(step, stress, SPEED_X, SPEED_Y, step + 1, STRESS_X, STRESS_Y, 2 + 2 * step)
    over(1, cx - 1, functools.partial(stress, final, inner))
    for way in (1, -1):
        receive_y(final, SPEED_Y, way)
    over(1, cx - 1, functools.partial(stress, final, outer))
    receive_words(final)
    over(1, cx - 1, functools.partial(gradient, final, False))
    ends(functools.partial(gradient, final, True))
    for piece in range(pieces):
        receive_x(final, SPEED_X, piece)
    finish_sends(final, SPEED_X, SPEED_Y)


def finish(cur, coef, halo_y, fwd, grads_in, out, grads, s_end, g_end, sem):
    cx, cy, cz = coef.shape[1:]
    tile, z_before, z_after, y_before, y_after, strains, stresses = stencil(cur, coef, halo_y)
    copies = []

    def send(source, target):
        copies.append(pltpu.make_async_copy(source, target, sem.at[len(copies)]))
        copies[-1].start()

    for field in (VX, VY, VZ):
        send(cur.at[field, pl.ds(1, cx)], out.at[field])
    middle = pl.ds(1, cx - 2)
    send(cur.at[pl.ds(SXX, 6), pl.ds(2, cx - 2)], out.at[pl.ds(SXX, 6), middle])
    send(grads_in.at[:, middle], grads.at[:, middle])
    for end, x in enumerate((0, cx - 1)):
        for t in range(cy // ROWS):
            rows = pl.ds(t * ROWS, ROWS)
            both = strains(STEPS - 1, x, t)
            for index, value in enumerate(stresses(both, x, t)):
                s_end[index, end, rows, :] = value
            f = [fwd[index, x, rows, :] for index in range(6)]
            for index, value in enumerate(products(both, f)):
                g_end[index, end, rows, :] = grads_in[index, x, rows, :] + value
        send(s_end.at[:, end], out.at[pl.ds(SXX, 6), x])
        send(g_end.at[:, end], grads.at[:, x])
    for copy in copies:
        copy.wait()


def on_device(n_x, n_y, adjoint, buoyancy, lame_lambda, shear_mu, packed, scales, perm):
    fields, cx, cy, cz = adjoint.shape
    comp, segw = packed.shape[3:]
    lanes = min(128, segw)
    packed = packed.reshape(n_x, comp, segw // lanes, lanes)
    halos = 6 * STEPS
    pieces = PIECES if cy % (PIECES * ROWS) == 0 else 1
    dma = pltpu.SemaphoreType.DMA
    held = pl.pallas_call(
        functools.partial(kernel, n_x, n_y),
        out_shape=(pltpu.VMEM((fields, cx + 2, cy, cz), jnp.float32), pltpu.VMEM((3, cx, cy, cz), jnp.float32),
                   pltpu.VMEM((halos, cx, cz), jnp.float32), pltpu.VMEM((6, cx, cy, cz), jnp.float32),
                   pltpu.VMEM((2, cx, cy, cz), jnp.float32)),
        in_specs=[pl.BlockSpec(memory_space=pltpu.HBM)] * 7,
        out_specs=(pl.BlockSpec(memory_space=pltpu.VMEM),) * 5,
        scratch_shapes=[
            pltpu.VMEM((comp, cx, cy, cz), jnp.float32),
            pltpu.VMEM((halos, cx, cz), jnp.float32),
            pltpu.VMEM((len(RELAYED), comp // STEPS, segw // lanes, lanes), jnp.int32),
            pltpu.VMEM((n_x, 1, comp), jnp.float32),
            pltpu.SMEM((n_x, 1, comp), jnp.float32),
            pltpu.SMEM(perm.shape, jnp.int32),
            pltpu.SMEM((n_x,), jnp.int32),
            dma((14,)), dma((len(RELAYED),)), dma((len(RELAYED),)), dma((halos, pieces)), dma((halos, pieces)), dma((halos,)), dma((halos,)),
            dma((n_x, STEPS)), dma((n_x, STEPS)), dma((n_x,)), dma((n_x,)), dma((3 + STEPS,)),
        ] + [pltpu.VMEM((n_x, comp // STEPS, segw // lanes, lanes), jnp.int32)] * STEPS,
        compiler_params=pltpu.CompilerParams(collective_id=0, has_side_effects=True,
                                             vmem_limit_bytes=VMEM_LIMIT),
    )(adjoint, buoyancy, lame_lambda, shear_mu, packed, scales, perm)
    return pl.pallas_call(
        finish,
        out_shape=(jax.ShapeDtypeStruct(adjoint.shape, jnp.float32), jax.ShapeDtypeStruct((2, cx, cy, cz), jnp.float32)),
        in_specs=[pl.BlockSpec(memory_space=pltpu.VMEM)] * 5,
        out_specs=(pl.BlockSpec(memory_space=pltpu.HBM),) * 2,
        scratch_shapes=[
            pltpu.VMEM((6, 2, cy, cz), jnp.float32),
            pltpu.VMEM((2, 2, cy, cz), jnp.float32),
            dma((9,)),
        ],
        compiler_params=pltpu.CompilerParams(vmem_limit_bytes=8000000),
    )(*held)


def solution(mesh):
    return jax.shard_map(
        functools.partial(on_device, mesh.shape["gx"], mesh.shape["gy"]),
        mesh=mesh,
        in_specs=(
            P(None, "gx", "gy", None),
            P("gx", "gy", None),
            P("gx", "gy", None),
            P("gx", "gy", None),
            P("gx", None, "gy", None, None),
            P("gx", None, "gy", None),
            P("gx", None),
        ),
        out_specs=(P(None, "gx", "gy", None), P(None, "gx", "gy", None)),
        check_vma=False,
    )
```
